32 devices in a mesh: seq: 8 (over z, x), head: 4 (over y, core).
Axes of the slice: x: 2, y: 2, z: 4, core: 2. Of those that a mesh axis runs over, the one named last changes fastest.
Arguments:
- query: bfloat16 [4096, 4096], P(('seq', 'head')), may hold values from -6 to 6
- key: bfloat16 [4096, 1024], P(('seq', 'head')), may hold values from -6 to 6
- value: bfloat16 [4096, 1024], P(('seq', 'head')), may hold values from -6 to 6
- out: bfloat16 [4096, 4096], P(('seq', 'head')), may hold values from -4 to 4
- output_gradient: bfloat16 [4096, 4096], P(('seq', 'head')), may hold values from -6 to 6
- log_sum_exp: float32 [4096, 32], P(('seq', 'head')), may hold values from 4 to 7
- segment_ids: int32 [4096], replicated, may hold values from 0 to 3, never falling along the last dimension, each value on 1 to 1536 neighbouring positions
Outputs:
- d_query: bfloat16 [4096, 4096], P(('seq', 'head'))
- key_gradient: bfloat16 [4096, 1024], P(('seq', 'head'))
- value_gradient: bfloat16 [4096, 1024], P(('seq', 'head'))
The draws below stay inside these ranges and needn't reach their ends.
Inputs may be any that keep to these rules, and one draw needn't show every extreme that they name: `segment_ids`: never falls along the positions; a document holds at most 1536 positions, and one holds exactly 1536.
All inputs are finite; a program needn't handle non-finite values.
Results may differ from the reference program's by a relative error of at most 0.0071.
Values may be sent and summed in bfloat16 or wider, within the bound.
A program may use at most 128 MiB of HBM per device.

```python
import math
import jax
import jax.numpy as jnp
import numpy as np
from jax import lax

QUERY_HEADS = 32
KEY_VALUE_HEADS = 8
HEAD_SIZE = 128
TOK_DEV = 128
REACH = 3
PACKED_TOKENS = 4096
MOST = 1536
DOCS = 4
N_HEAD = 4


def block_levels(rng, shape, pieces, low, top_value):
    level, own = 1.0, jax.random.fold_in(rng, 6)
    for axis_at, shards_of in pieces:
        heights = jnp.exp(jax.random.uniform(jax.random.fold_in(own, axis_at), (shards_of,), jnp.float32, low / len(pieces), top_value / len(pieces)))
        level = level * jnp.repeat(heights, shape[axis_at] // shards_of).reshape([-1 if axis == axis_at else 1 for axis in range(len(shape))])
    return level


def split_up(number_of, total, most, slope):
    portions = [(1 << 20) // math.isqrt(rank ** slope) + 1 for rank in range(2, number_of + 1)]
    spare, counts = total - most - (number_of - 1), [1] * (number_of - 1)
    while spare > 0:
        movable = [i for i in range(number_of - 1) if counts[i] < most]
        pool, budget = sum([portions[i] for i in movable]), spare
        for i in movable:
            more = min(most - counts[i], max(1, budget * portions[i] // pool), spare)
            counts[i] = counts[i] + more
            spare = spare - more
    return np.array([most] + counts)


def uneven_parts(key, number_of, total, most, lean):
    if number_of == 2:
        one = jax.random.randint(key, (), max(1, total - most), min(most, total - 1) + 1)
        return jnp.stack([one, total - one])
    sizes = jnp.asarray(split_up(number_of, total, most, lean), jnp.int32)
    couples = (number_of - 1) // 2
    donor, sink = sizes[1:1 + 2 * couples:2], sizes[2:2 + 2 * couples:2]
    slack = jnp.minimum(donor - 1, most - sink)
    moved = jax.random.randint(jax.random.fold_in(key, 1), (couples,), 0, 1 << 20) % (slack + 1)
    sizes = sizes.at[1:1 + 2 * couples:2].set(donor - moved).at[2:2 + 2 * couples:2].set(sink + moved)
    return sizes[jax.random.permutation(jax.random.fold_in(key, 2), number_of)]


def noise(rng, shape, width, bound, cuts=(), kind=jnp.bfloat16):
    level = block_levels(rng, shape, cuts, -0.22, 0.18) if cuts else 1.0
    entries = jax.random.normal(rng, shape, jnp.float32) * width * level
    return jnp.minimum(jnp.maximum(entries, -bound), bound).astype(kind)


def setup_inputs(seed: int = 0) -> dict:
    streams_of = jax.random.split(jax.random.key(seed), 8)
    query = noise(streams_of[0], (PACKED_TOKENS, QUERY_HEADS * HEAD_SIZE), 1.0, 6.0, ((0, 32),))
    key = noise(streams_of[1], (PACKED_TOKENS, KEY_VALUE_HEADS * HEAD_SIZE), 1.0, 6.0, ((0, 32),))
    value = noise(streams_of[2], (PACKED_TOKENS, KEY_VALUE_HEADS * HEAD_SIZE), 1.0, 6.0, ((0, 32),))
    out = noise(streams_of[3], (PACKED_TOKENS, QUERY_HEADS * HEAD_SIZE), 0.5, 4.0, ((0, 32),))
    output_gradient = noise(streams_of[4], (PACKED_TOKENS, QUERY_HEADS * HEAD_SIZE), 1.0, 6.0, ((0, 32),))
    log_sum_exp = jnp.clip(4.0 + 3.0 * jax.random.uniform(streams_of[5], (PACKED_TOKENS, QUERY_HEADS), jnp.float32) ** block_levels(streams_of[5], (PACKED_TOKENS, QUERY_HEADS), ((0, 32),), -0.2, 0.2), 4.0, 7.0)
    segment_ids = jnp.searchsorted(jnp.cumsum(uneven_parts(streams_of[6], DOCS, PACKED_TOKENS, MOST, 2)), jnp.arange(PACKED_TOKENS), side="right").astype(jnp.int32)
    return {"query": query, "key": key, "value": value, "out": out, "output_gradient": output_gradient, "log_sum_exp": log_sum_exp, "segment_ids": segment_ids}


def rounded(values):
    return lax.optimization_barrier(values.astype(jnp.bfloat16)).astype(jnp.float32)

def reference(query, key, value, out, output_gradient, log_sum_exp, segment_ids):
    row_number = TOK_DEV * N_HEAD
    block_list = PACKED_TOKENS // row_number
    group_width = QUERY_HEADS // KEY_VALUE_HEADS
    score_scale = 1.0 / math.sqrt(HEAD_SIZE)
    padding_rows = REACH * row_number
    window_rows = (REACH + 1) * row_number
    query_total = query.astype(jnp.float32).reshape(block_list, row_number, KEY_VALUE_HEADS, group_width, HEAD_SIZE)
    gradient_total = output_gradient.astype(jnp.float32).reshape(block_list, row_number, KEY_VALUE_HEADS, group_width, HEAD_SIZE)
    output_total = out.astype(jnp.float32).reshape(block_list, row_number, KEY_VALUE_HEADS, group_width, HEAD_SIZE)
    delta_all = lax.optimization_barrier(jnp.sum(gradient_total * output_total, axis=4))
    log_sum_exp_total = log_sum_exp.astype(jnp.float32).reshape(block_list, row_number, KEY_VALUE_HEADS, group_width)
    key_padded = jnp.concatenate([jnp.zeros((padding_rows, KEY_VALUE_HEADS * HEAD_SIZE), jnp.float32), key.astype(jnp.float32)], axis=0).reshape(padding_rows + PACKED_TOKENS, KEY_VALUE_HEADS, HEAD_SIZE)
    value_padded = jnp.concatenate([jnp.zeros((padding_rows, KEY_VALUE_HEADS * HEAD_SIZE), jnp.float32), value.astype(jnp.float32)], axis=0).reshape(padding_rows + PACKED_TOKENS, KEY_VALUE_HEADS, HEAD_SIZE)
    seg_ids = segment_ids.astype(jnp.int32)
    seg_pad = jnp.concatenate([jnp.full((padding_rows,), -1, jnp.int32), seg_ids])
    query_offsets = jnp.arange(row_number, dtype=jnp.int32) + padding_rows
    key_offsets = jnp.arange(window_rows, dtype=jnp.int32)

    def block_step(accums, inputs):
        key_gradient_total, value_gradient_total = accums
        query_heads, grad_heads, delta_rows, lse_rows, index = inputs
        window_start = (index * row_number).astype(jnp.int32)
        key_block = lax.dynamic_slice_in_dim(key_padded, window_start, window_rows, 0)
        value_block = lax.dynamic_slice_in_dim(value_padded, window_start, window_rows, 0)
        seg_keys = lax.dynamic_slice_in_dim(seg_pad, window_start, window_rows, 0)
        seg_query = lax.dynamic_slice_in_dim(seg_ids, window_start, row_number, 0)
        allowed = (seg_query[:, None] == seg_keys[None, :]) & (key_offsets[None, :] <= query_offsets[:, None])
        lse_cols = lse_rows.transpose(1, 2, 0)[..., None]
        delta_cols = delta_rows.transpose(1, 2, 0)[..., None]
        scores = jnp.einsum('igmd,jgd->gmij', query_heads, key_block) * score_scale
        probs = jnp.exp(jnp.where(allowed, scores - lse_cols, -jnp.inf))
        probs_low = rounded(probs)
        dprobs = jnp.einsum('igmd,jgd->gmij', grad_heads, value_block)
        dscores = rounded(score_scale * probs * (dprobs - delta_cols))
        grad_query = jnp.einsum('gmij,jgd->igmd', dscores, key_block)
        grad_key = jnp.einsum('gmij,igmd->jgd', dscores, query_heads)
        grad_value = jnp.einsum('gmij,igmd->jgd', probs_low, grad_heads)
        key_gradient_total = lax.dynamic_update_slice_in_dim(key_gradient_total, lax.dynamic_slice_in_dim(key_gradient_total, window_start, window_rows, 0) + grad_key, window_start, 0)
        value_gradient_total = lax.dynamic_update_slice_in_dim(value_gradient_total, lax.dynamic_slice_in_dim(value_gradient_total, window_start, window_rows, 0) + grad_value, window_start, 0)
        return ((key_gradient_total, value_gradient_total), grad_query.astype(jnp.bfloat16))
    starting_totals = (jnp.zeros((padding_rows + PACKED_TOKENS, KEY_VALUE_HEADS, HEAD_SIZE), jnp.float32), jnp.zeros((padding_rows + PACKED_TOKENS, KEY_VALUE_HEADS, HEAD_SIZE), jnp.float32))
    indices = jnp.arange(block_list, dtype=jnp.int32)
    (key_gradient_total, value_gradient_total), grad_blocks = lax.scan(block_step, starting_totals, (query_total, gradient_total, delta_all, log_sum_exp_total, indices))
    d_query = grad_blocks.reshape(PACKED_TOKENS, QUERY_HEADS * HEAD_SIZE)
    key_gradient = key_gradient_total[padding_rows:].reshape(PACKED_TOKENS, KEY_VALUE_HEADS * HEAD_SIZE).astype(jnp.bfloat16)
    value_gradient = value_gradient_total[padding_rows:].reshape(PACKED_TOKENS, KEY_VALUE_HEADS * HEAD_SIZE).astype(jnp.bfloat16)
    return (d_query, key_gradient, value_gradient)
```

```python
import functools
import math

import jax
import jax.numpy as jnp
from jax import lax
from jax.experimental import pallas as pl
from jax.experimental.pallas import tpu as pltpu
from jax.sharding import PartitionSpec as P

HEAD_SIZE = 128
BACK = 6
LOG2E = math.log2(math.e)
MESH = pl.DeviceIdType.MESH
NT = (((1,), (1,)), ((), ()))


def dot(a, b):
    return jnp.dot(a, b, preferred_element_type=jnp.float32)


def dot_nt(a, b):
    return lax.dot_general(a, b, NT, preferred_element_type=jnp.float32)


def kernel(
    n, seqs, width,
    q_ref, e_ref, o_ref, k_ref, v_ref, lse_ref, seg_ref,
    dq_out, dk_out, dv_out,
    qb, eb, stl, stb, kvb, segk, segq, dqt, acck, accv, ps, pr, dqs, dks, dvs,
    loc_sem, in_s, in_r, fw_s, fw_r, pt_s, pt_r, out_s, out_r,
):
    s = lax.axis_index("seq")
    h = lax.axis_index("head")
    rows = q_ref.shape[0]
    hd = HEAD_SIZE
    tile = 2 * rows
    size = 2 * n
    tiles = size // 2
    window = tiles + BACK
    cols = width * hd
    pairs = width // 2
    pcols = cols // pairs
    scale = 1.0 / math.sqrt(hd)
    f32, bf16 = jnp.float32, jnp.bfloat16

    def at(index, length):
        return pl.ds(index * length if isinstance(index, int) else pl.multiple_of(index * length, length), length)

    plane = s // 2
    p = lax.rem(s, 2) * n + h
    own = p // 2
    has_up, has_down, has_two = s + 2 < seqs, s >= 2, s >= 4

    def dev(index):
        return {"seq": s - lax.rem(s, 2) + index // n, "head": lax.rem(index, n)}

    def flip(value, by):
        bit = 1
        while bit <= by:
            if (by // bit) % 2:
                value = value + bit - 2 * bit * lax.rem(value // bit, 2)
            bit *= 2
        return value

    barrier = pltpu.get_barrier_semaphore()
    for by in range(1, size):
        pl.semaphore_signal(barrier, inc=1, device_id=dev(flip(p, by)), device_id_type=MESH)

    @pl.when(has_up)
    def _():
        pl.semaphore_signal(barrier, inc=1, device_id={"seq": s + 2}, device_id_type=MESH)

    @pl.when(has_down)
    def _():
        pl.semaphore_signal(barrier, inc=1, device_id={"seq": s - 2}, device_id_type=MESH)

    pl.semaphore_wait(barrier, size - 1 + jnp.minimum(s // 2, 1) + jnp.minimum((seqs - 1 - s) // 2, 1))

    kinds = 3 + 2 * pairs

    def entry(kind, to, me):
        if kind < 2:
            dst = kvb.at[BACK + me // 2, kind, at(lax.rem(me, 2), rows), :]
            return (k_ref, v_ref)[kind].at[:, at(to, hd)], dst
        if kind == 2:
            return stl.at[to], stb.at[:, at(me, rows)]
        pair, which = (kind - 3) // 2, (kind - 3) % 2
        src = (q_ref, e_ref)[which].at[:, at(to * pairs + pair, pcols)]
        return src, (qb, eb)[which].at[at(me, rows), pl.ds(pair * pcols, pcols)]

    def entry_copy(kind, to):
        src, dst = entry(kind, to, p)
        return pltpu.make_async_remote_copy(
            src_ref=src, dst_ref=dst, send_sem=in_s.at[kind, to], recv_sem=in_r.at[kind, p],
            device_id=dev(to), device_id_type=MESH)

    def entry_got(kind, by):
        _, dst = entry(kind, p, flip(p, by))
        pltpu.make_async_remote_copy(
            src_ref=dst, dst_ref=dst, send_sem=in_s.at[kind, flip(p, by)], recv_sem=in_r.at[kind, flip(p, by)],
            device_id=dev(flip(p, by)), device_id_type=MESH).wait_recv()

    def entry_own(kind):
        src, dst = entry(kind, p, p)
        return pltpu.make_async_copy(src, dst, loc_sem.at[kind])

    order = tuple(sorted(range(1, size), key=lambda by: (by // 2 > 0, by // 2 == 3, by % 2, by)))

    for kind in (0, 1) + tuple(range(3, kinds)):
        entry_own(kind).start()
    for by in order:
        for kind in (0, 1):
            entry_copy(kind, flip(p, by)).start()

    lane = lax.broadcasted_iota(jnp.int32, (rows, hd), 1)
    delta = jnp.zeros((rows, hd), f32)
    for head in range(width * size):
        here = pl.ds(head * hd, hd)
        one = jnp.sum(e_ref[:, here].astype(f32) * o_ref[:, here].astype(f32), axis=1, keepdims=True)
        delta = jnp.where(lane == head, one, delta)
    delta = delta.T
    for to in range(size):
        stl[to, :width, :] = lse_ref[to * width : (to + 1) * width, :] * LOG2E
        stl[to, width:, :] = delta[to * width : (to + 1) * width, :]
    entry_own(2).start()
    for by in order:
        entry_copy(2, flip(p, by)).start()
    for kind in range(3, kinds):
        entry_copy(kind, flip(p, 1)).start()
    for pair in range(pairs):
        for by in order[1:]:
            for which in range(2):
                entry_copy(3 + 2 * pair + which, flip(p, by)).start()

    first = plane * size - BACK * 2
    for a in range(2 * window):
        row = seg_ref[pl.ds(jnp.maximum(first + a, 0), 1), :].astype(f32)
        segk[a * rows : (a + 1) * rows, :] = jnp.broadcast_to(row, (rows, hd)).T
        if a >= 2 * BACK:
            segq[:, (a - 2 * BACK) * rows : (a - 2 * BACK + 1) * rows] = row
    dqt[...] = jnp.zeros_like(dqt)
    acck[...] = jnp.zeros_like(acck)
    accv[...] = jnp.zeros_like(accv)

    def hand(w):
        return pltpu.make_async_remote_copy(
            src_ref=kvb.at[w + tiles], dst_ref=kvb.at[w], send_sem=fw_s.at[w], recv_sem=fw_r.at[w],
            device_id={"seq": s + 2}, device_id_type=MESH)

    def back(w):
        return pltpu.make_async_remote_copy(
            src_ref=ps.at[w], dst_ref=pr.at[w], send_sem=pt_s.at[w], recv_sem=pt_r.at[w],
            device_id={"seq": s - 2}, device_id_type=MESH)

    row_at = lax.broadcasted_iota(jnp.int32, (tile, tile), 0)
    col_at = lax.broadcasted_iota(jnp.int32, (tile, tile), 1)

    def work(i, w, pair):
        q_rows = at(i, tile)
        key, val = kvb[w, 0], kvb[w, 1]
        key_t = key.T
        k_seg = segk[at(w, tile), :]
        allowed = jnp.concatenate([k_seg] * (tile // hd), axis=1) == segq[:, q_rows]
        if not isinstance(w, int) or w >= BACK:
            allowed &= row_at + (w - BACK - i) * tile <= col_at
        mine = range(pair * width // pairs, (pair + 1) * width // pairs)
        queries = [qb[q_rows, m * hd : (m + 1) * hd] for m in mine]
        grads = [eb[q_rows, m * hd : (m + 1) * hd] for m in mine]
        scores = [dot_nt(key, query) for query in queries]
        dprobs = [dot_nt(val, grad) for grad in grads]
        low, dscores = [], []
        for m, score, dprob in zip(mine, scores, dprobs):
            lse = stb[m : m + 1, q_rows]
            delta = stb[width + m : width + m + 1, q_rows]
            probs = jnp.exp2(jnp.where(allowed, score * (scale * LOG2E) - lse, -jnp.inf))
            low.append(probs.astype(bf16))
            dscores.append((probs * (dprob - delta)).astype(bf16))
        accv[w] += dot(jnp.concatenate(low, axis=1), jnp.concatenate(grads, axis=0))
        acck[w] += dot(jnp.concatenate(dscores, axis=1), jnp.concatenate(queries, axis=0))
        for m, dscore in zip(mine, dscores):
            dqt[i, m] += dot(key_t, dscore)

    def leave(which, to, me):
        if which < pairs:
            src = dqs.at[at(to, rows), pl.ds(which * pcols, pcols)]
            return src, dq_out.at[:, at(me * pairs + which, pcols)]
        src, dst = ((dks, dk_out), (dvs, dv_out))[which - pairs]
        return src.at[at(to, rows), :], dst.at[:, at(me, hd)]

    leaves = pairs + 2

    def leave_copy(which, to):
        src, dst = leave(which, to, p)
        return pltpu.make_async_remote_copy(
            src_ref=src, dst_ref=dst, send_sem=out_s.at[which, to], recv_sem=out_r.at[which, p],
            device_id=dev(to), device_id_type=MESH)

    def leave_got(which, by):
        _, dst = leave(which, p, flip(p, by))
        pltpu.make_async_remote_copy(
            src_ref=dst, dst_ref=dst, send_sem=out_s.at[which, flip(p, by)], recv_sem=out_r.at[which, flip(p, by)],
            device_id=dev(flip(p, by)), device_id_type=MESH).wait_recv()

    def leave_own(which):
        src, dst = leave(which, p, p)
        return pltpu.make_async_copy(src, dst, loc_sem.at[kinds + which])

    def leave_start(which, i):
        for b in range(2):
            to = 2 * i + b

            @pl.when(to != p)
            def _():
                leave_copy(which, to).start()

            @pl.when(to == p)
            def _():
                leave_own(which).start()

    def leave_query(i, pair):
        for m in range(pair * width // pairs, (pair + 1) * width // pairs):
            dqs[at(i, tile), m * hd : (m + 1) * hd] = (dqt[i, m] * scale).T.astype(bf16)
        leave_start(pair, i)

    entry_own(2).wait()
    for kind in range(2, kinds):
        if kind > 2:
            entry_own(kind).wait()
    entry_own(0).wait()
    entry_own(1).wait()
    for j in range(tiles):
        for by in range(max(2 * j, 1), 2 * j + 2):
            entry_got(0, by)
            entry_got(1, by)
        t = flip(own, j)

        @pl.when(has_up)
        def _():
            hand(t + BACK - tiles).start()

        if j == 0:
            for kind in range(2, kinds):
                entry_got(kind, 1)

        @pl.when(t <= own)
        def _():
            for pair in range(pairs):
                work(own, t + BACK, pair)

    for j in range(1, tiles):
        for by in range(2 * j, 2 * j + 2):
            for kind in (2, 3, 4):
                entry_got(kind, by)
        i = flip(own, j)

        @pl.loop(0, i + 1)
        def _(t):
            work(i, t + BACK, 0)

    @pl.when(has_down)
    def _():
        for w in range(BACK - 1, BACK - tiles - 1, -1):
            hand(w).wait_recv()
            if w >= tiles:
                @pl.when(has_up)
                def _():
                    hand(w - tiles).start()

            @pl.loop(0, min(tiles - 1, w) + 1)
            def _(i):
                work(i, w, 0)

            @pl.when(own <= w)
            def _():
                for pair in range(1, pairs):
                    work(own, w, pair)

    for i in range(BACK - tiles, tiles):
        leave_query(i, 0)

    @pl.when(has_two)
    def _():
        for w in range(BACK - tiles - 1, -1, -1):
            hand(w).wait_recv()

            @pl.loop(0, w + 1)
            def _(i):
                work(i, w, 0)

            @pl.when(own <= w)
            def _():
                for pair in range(1, pairs):
                    work(own, w, pair)

    for i in range(BACK - tiles):
        leave_query(i, 0)
    for pair in range(1, pairs):
        leave_query(own, pair)

    for j in range(1, tiles):
        for by in range(2 * j, 2 * j + 2):
            for kind in range(5, kinds):
                entry_got(kind, by)

    def rest(w):
        @pl.loop(max(w - BACK, 0), min(tiles - 1, w) + 1)
        def _(i):
            @pl.when(i != own)
            def _():
                for pair in range(1, pairs):
                    work(i, w, pair)

    def put(w):
        ps[w, 0] = acck[w].astype(bf16)
        ps[w, 1] = accv[w].astype(bf16)
        back(w).start()

    def join(w):
        back(w - tiles).wait_recv()
        acck[w] += pr[w - tiles, 0].astype(f32)
        accv[w] += pr[w - tiles, 1].astype(f32)

    @pl.when(has_two)
    def _():
        for w in range(BACK - tiles):
            rest(w)
            put(w)

    @pl.when(has_down)
    def _():
        for w in range(BACK - tiles, BACK):
            rest(w)
            if w < tiles:
                put(w)

    for w in range(BACK, window):
        rest(w)
        for pair in range(1, pairs):
            @pl.when(w - BACK != own)
            def _():
                leave_query(w - BACK, pair)

    @pl.when(has_down)
    def _():
        for w in range(tiles, BACK):
            @pl.when(has_up)
            def _():
                join(w)

            put(w)

    for w in range(BACK, window):
        @pl.when(has_up)
        def _():
            join(w)

        t = w - BACK
        dks[t * tile : (t + 1) * tile, :] = (acck[w] * scale).astype(bf16)
        dvs[t * tile : (t + 1) * tile, :] = accv[w].astype(bf16)
        leave_start(pairs, t)
        leave_start(pairs + 1, t)

    for which in range(leaves):
        leave_own(which).wait()
        for by in range(1, size):
            leave_got(which, by)
            leave_copy(which, flip(p, by)).wait_send()
    for kind in range(kinds):
        for by in range(1, size):
            entry_copy(kind, flip(p, by)).wait_send()
    for w in range(BACK):
        low = w < BACK - tiles

        @pl.when(has_up & has_down if low else has_up)
        def _():
            hand(w).wait_send()

        @pl.when(has_two if low else has_down)
        def _():
            back(w).wait_send()


def shards(query, key, value, out, output_gradient, log_sum_exp, segment_ids):
    n, seqs = lax.axis_size("head"), lax.axis_size("seq")
    hd = HEAD_SIZE
    rows = query.shape[0]
    size = 2 * n
    cols = query.shape[1] // size
    width = cols // hd
    pairs = width // 2
    tile, tiles = 2 * rows, size // 2
    window = tiles + BACK
    bf16, f32 = jnp.bfloat16, jnp.float32
    kinds, leaves = 3 + 2 * pairs, pairs + 2
    vmem = pl.BlockSpec(memory_space=pltpu.VMEM)
    dma = pltpu.SemaphoreType.DMA
    return pl.pallas_call(
        functools.partial(kernel, n, seqs, width),
        out_shape=[
            jax.ShapeDtypeStruct(query.shape, bf16),
            jax.ShapeDtypeStruct(key.shape, bf16),
            jax.ShapeDtypeStruct(value.shape, bf16),
        ],
        in_specs=[vmem] * 7,
        out_specs=[vmem] * 3,
        scratch_shapes=[
            pltpu.VMEM((size * rows, cols), bf16),
            pltpu.VMEM((size * rows, cols), bf16),
            pltpu.VMEM((size, 2 * width, rows), f32),
            pltpu.VMEM((2 * width, size * rows), f32),
            pltpu.VMEM((window, 2, tile, hd), bf16),
            pltpu.VMEM((window * tile, hd), f32),
            pltpu.VMEM((1, size * rows), f32),
            pltpu.VMEM((tiles, width, hd, tile), f32),
            pltpu.VMEM((window, tile, hd), f32),
            pltpu.VMEM((window, tile, hd), f32),
            pltpu.VMEM((BACK, 2, tile, hd), bf16),
            pltpu.VMEM((BACK, 2, tile, hd), bf16),
            pltpu.VMEM((size * rows, cols), bf16),
            pltpu.VMEM((size * rows, hd), bf16),
            pltpu.VMEM((size * rows, hd), bf16),
            dma((kinds + leaves,)),
            dma((kinds, size)),
            dma((kinds, size)),
            dma((BACK,)),
            dma((BACK,)),
            dma((BACK,)),
            dma((BACK,)),
            dma((leaves, size)),
            dma((leaves, size)),
        ],
        compiler_params=pltpu.CompilerParams(collective_id=0, has_side_effects=True),
    )(query, output_gradient, out, key, value, log_sum_exp.T, segment_ids.reshape(-1, hd))


def solution(mesh):
    placed = (P(("seq", "head"), None),) * 6 + (P(),)
    return jax.shard_map(
        lambda *a: tuple(shards(*a)),
        mesh=mesh,
        in_specs=placed,
        out_specs=(P(("seq", "head"), None),) * 3,
        check_vma=False,
    )
```

```python
import functools
import math

import jax
import jax.numpy as jnp
from jax import lax
from jax.experimental import pallas as pl
from jax.experimental.pallas import tpu as pltpu
from jax.sharding import PartitionSpec as P

HEAD_SIZE = 128
BACK = 6
LOG2E = math.log2(math.e)
MESH = pl.DeviceIdType.MESH
NT = (((1,), (1,)), ((), ()))


def dot(a, b):
    return jnp.dot(a, b, preferred_element_type=jnp.float32)


def dot_nt(a, b):
    return lax.dot_general(a, b, NT, preferred_element_type=jnp.float32)


def kernel(
    n, seqs, width,
    q_in, e_in, o_in, k_in, v_in, lse_ref, seg_ref,
    dq_out, dk_out, dv_out,
    k_ref, v_ref, e_ref, o_ref, q_ref, load_sem, qb, eb, stl, stb, kvb, segk, segq, dqt, acck, accv, ps, pr, dqs, dks, dvs,
    loc_sem, in_s, in_r, fw_s, fw_r, pt_s, pt_r, out_s, out_r,
):
    s = lax.axis_index("seq")
    h = lax.axis_index("head")
    rows = q_ref.shape[0]
    hd = HEAD_SIZE
    loads = [
        pltpu.make_async_copy(src, dst, load_sem.at[at])
        for at, (src, dst) in enumerate(((k_in, k_ref), (v_in, v_ref), (e_in, e_ref), (o_in, o_ref), (q_in, q_ref)))
    ]
    for load in loads:
        load.start()
    tile = 2 * rows
    size = 2 * n
    tiles = size // 2
    window = tiles + BACK
    cols = width * hd
    pairs = width // 2
    pcols = cols // pairs
    scale = 1.0 / math.sqrt(hd)
    f32, bf16 = jnp.float32, jnp.bfloat16

    def at(index, length):
        return pl.ds(index * length if isinstance(index, int) else pl.multiple_of(index * length, length), length)

    plane = s // 2
    p = lax.rem(s, 2) * n + h
    own = p // 2
    has_up, has_down, has_two = s + 2 < seqs, s >= 2, s >= 4

    def dev(index):
        return {"seq": s - lax.rem(s, 2) + index // n, "head": lax.rem(index, n)}

    def flip(value, by):
        bit = 1
        while bit <= by:
            if (by // bit) % 2:
                value = value + bit - 2 * bit * lax.rem(value // bit, 2)
            bit *= 2
        return value

    barrier = pltpu.get_barrier_semaphore()
    for by in range(1, size):
        pl.semaphore_signal(barrier, inc=1, device_id=dev(flip(p, by)), device_id_type=MESH)

    @pl.when(has_up)
    def _():
        pl.semaphore_signal(barrier, inc=1, device_id={"seq": s + 2}, device_id_type=MESH)

    @pl.when(has_down)
    def _():
        pl.semaphore_signal(barrier, inc=1, device_id={"seq": s - 2}, device_id_type=MESH)

    pl.semaphore_wait(barrier, size - 1 + jnp.minimum(s // 2, 1) + jnp.minimum((seqs - 1 - s) // 2, 1))

    kinds = 3 + 2 * pairs

    def entry(kind, to, me):
        if kind < 2:
            dst = kvb.at[BACK + me // 2, kind, at(lax.rem(me, 2), rows), :]
            return (k_ref, v_ref)[kind].at[:, at(to, hd)], dst
        if kind == 2:
            return stl.at[to], stb.at[:, at(me, rows)]
        pair, which = (kind - 3) // 2, (kind - 3) % 2
        src = (q_ref, e_ref)[which].at[:, at(to * pairs + pair, pcols)]
        return src, (qb, eb)[which].at[at(me, rows), pl.ds(pair * pcols, pcols)]

    def entry_copy(kind, to):
        src, dst = entry(kind, to, p)
        return pltpu.make_async_remote_copy(
            src_ref=src, dst_ref=dst, send_sem=in_s.at[kind, to], recv_sem=in_r.at[kind, p],
            device_id=dev(to), device_id_type=MESH)

    def entry_got(kind, by):
        _, dst = entry(kind, p, flip(p, by))
        pltpu.make_async_remote_copy(
            src_ref=dst, dst_ref=dst, send_sem=in_s.at[kind, flip(p, by)], recv_sem=in_r.at[kind, flip(p, by)],
            device_id=dev(flip(p, by)), device_id_type=MESH).wait_recv()

    def entry_own(kind):
        src, dst = entry(kind, p, p)
        return pltpu.make_async_copy(src, dst, loc_sem.at[kind])

    order = tuple(sorted(range(1, size), key=lambda by: (by // 2 > 0, by // 2 == 3, by % 2, by)))

    for kind in (0, 1):
        loads[kind].wait()
        entry_own(kind).start()
    for by in order:
        for kind in (0, 1):
            entry_copy(kind, flip(p, by)).start()
    loads[2].wait()
    loads[3].wait()

    lane = lax.broadcasted_iota(jnp.int32, (rows, hd), 1)
    delta = jnp.zeros((rows, hd), f32)
    for head in range(width * size):
        here = pl.ds(head * hd, hd)
        one = jnp.sum(e_ref[:, here].astype(f32) * o_ref[:, here].astype(f32), axis=1, keepdims=True)
        delta = jnp.where(lane == head, one, delta)
    delta = delta.T
    for to in range(size):
        stl[to, :width, :] = lse_ref[to * width : (to + 1) * width, :] * LOG2E
        stl[to, width:, :] = delta[to * width : (to + 1) * width, :]
    entry_own(2).start()
    for by in order:
        entry_copy(2, flip(p, by)).start()
    loads[4].wait()
    for kind in range(3, kinds):
        entry_own(kind).start()
        entry_copy(kind, flip(p, 1)).start()
    for near in (order[1:5], order[5:]):
        for kind in range(3, kinds):
            for by in near:
                entry_copy(kind, flip(p, by)).start()

    first = plane * size - BACK * 2
    for a in range(2 * window):
        row = seg_ref[pl.ds(jnp.maximum(first + a, 0), 1), :].astype(f32)
        segk[a * rows : (a + 1) * rows, :] = jnp.broadcast_to(row, (rows, hd)).T
        if a >= 2 * BACK:
            segq[:, (a - 2 * BACK) * rows : (a - 2 * BACK + 1) * rows] = row
    dqt[...] = jnp.zeros_like(dqt)
    acck[...] = jnp.zeros_like(acck)
    accv[...] = jnp.zeros_like(accv)

    def hand(w):
        return pltpu.make_async_remote_copy(
            src_ref=kvb.at[w + tiles], dst_ref=kvb.at[w], send_sem=fw_s.at[w], recv_sem=fw_r.at[w],
            device_id={"seq": s + 2}, device_id_type=MESH)

    def back(w):
        return pltpu.make_async_remote_copy(
            src_ref=ps.at[w], dst_ref=pr.at[w], send_sem=pt_s.at[w], recv_sem=pt_r.at[w],
            device_id={"seq": s - 2}, device_id_type=MESH)

    row_at = lax.broadcasted_iota(jnp.int32, (tile, tile), 0)
    col_at = lax.broadcasted_iota(jnp.int32, (tile, tile), 1)

    def work(i, w, pair):
        q_rows = at(i, tile)
        key, val = kvb[w, 0], kvb[w, 1]
        key_t = key.T
        k_seg = segk[at(w, tile), :]
        allowed = jnp.concatenate([k_seg] * (tile // hd), axis=1) == segq[:, q_rows]
        if not isinstance(w, int) or w >= BACK:
            allowed &= row_at + (w - BACK - i) * tile <= col_at
        mine = range(pair * width // pairs, (pair + 1) * width // pairs)
        queries = [qb[q_rows, m * hd : (m + 1) * hd] for m in mine]
        grads = [eb[q_rows, m * hd : (m + 1) * hd] for m in mine]
        scores = [dot_nt(key, query) for query in queries]
        dprobs = [dot_nt(val, grad) for grad in grads]
        low, dscores = [], []
        for m, score, dprob in zip(mine, scores, dprobs):
            lse = stb[m : m + 1, q_rows]
            delta = stb[width + m : width + m + 1, q_rows]
            probs = jnp.exp2(jnp.where(allowed, score * (scale * LOG2E) - lse, -jnp.inf))
            low.append(probs.astype(bf16))
            dscores.append((probs * (dprob - delta)).astype(bf16))
        accv[w] += dot(jnp.concatenate(low, axis=1), jnp.concatenate(grads, axis=0))
        acck[w] += dot(jnp.concatenate(dscores, axis=1), jnp.concatenate(queries, axis=0))
        for m, dscore in zip(mine, dscores):
            dqt[i, m] += dot(key_t, dscore)

    def leave(which, to, me):
        if which < pairs:
            src = dqs.at[at(to, rows), pl.ds(which * pcols, pcols)]
            return src, dq_out.at[:, at(me * pairs + which, pcols)]
        src, dst = ((dks, dk_out), (dvs, dv_out))[which - pairs]
        return src.at[at(to, rows), :], dst.at[:, at(me, hd)]

    leaves = pairs + 2

    def leave_copy(which, to):
        src, dst = leave(which, to, p)
        return pltpu.make_async_remote_copy(
            src_ref=src, dst_ref=dst, send_sem=out_s.at[which, to], recv_sem=out_r.at[which, p],
            device_id=dev(to), device_id_type=MESH)

    def leave_got(which, by):
        _, dst = leave(which, p, flip(p, by))
        pltpu.make_async_remote_copy(
            src_ref=dst, dst_ref=dst, send_sem=out_s.at[which, flip(p, by)], recv_sem=out_r.at[which, flip(p, by)],
            device_id=dev(flip(p, by)), device_id_type=MESH).wait_recv()

    def leave_own(which):
        src, dst = leave(which, p, p)
        return pltpu.make_async_copy(src, dst, loc_sem.at[kinds + which])

    def leave_start(which, i):
        for b in range(2):
            to = 2 * i + b

            @pl.when(to != p)
            def _():
                leave_copy(which, to).start()

            @pl.when(to == p)
            def _():
                leave_own(which).start()

    def fill(i):
        for m in range(width):
            dqs[at(i, tile), m * hd : (m + 1) * hd] = (dqt[i, m] * scale).T.astype(bf16)

    def all_pairs(i, w):
        for pair in range(pairs):
            work(i, w, pair)

    def query_got(j, pair):
        for by in range(2 * j, 2 * j + 2):
            for kind in ((2,) if pair == 0 else ()) + (3 + 2 * pair, 4 + 2 * pair):
                entry_got(kind, by)

    def put(w):
        ps[w, 0] = acck[w].astype(bf16)
        ps[w, 1] = accv[w].astype(bf16)
        back(w).start()

    def join(w):
        back(w - tiles).wait_recv()
        acck[w] += pr[w - tiles, 0].astype(f32)
        accv[w] += pr[w - tiles, 1].astype(f32)

    for kind in range(kinds):
        entry_own(kind).wait()
    for j in range(tiles):
        for by in range(max(2 * j, 1), 2 * j + 2):
            entry_got(0, by)
            entry_got(1, by)
        t = flip(own, j)

        @pl.when(has_up)
        def _():
            hand(t + BACK - tiles).start()

        if j == 0:
            for kind in range(2, kinds):
                entry_got(kind, 1)

        @pl.when(t <= own)
        def _():
            all_pairs(own, t + BACK)

    last = tiles - 1
    far = flip(own, last)

    def before(j):
        w = BACK - tiles + flip(own, j)

        @pl.when(has_down)
        def _():
            hand(w).wait_recv()

            @pl.when(has_up & (w >= tiles))
            def _():
                hand(w - tiles).start()

            @pl.when(own <= w)
            def _():
                all_pairs(own, w)

    def near(w, pair):
        @pl.loop(0, min(tiles - 1, w) + 1)
        def _(i):
            @pl.when((i != far) & (i != own))
            def _():
                work(i, w, pair)

    for j in range(last):
        before(j)
    for pair in range(pairs):
        for j in range(1, last):
            query_got(j, pair)
            i = flip(own, j)

            @pl.loop(0, i + 1)
            def _(t):
                work(i, t + BACK, pair)

        if pair == 0:
            before(last)

        @pl.when(has_down)
        def _():
            for w in range(BACK - tiles, BACK):
                near(w, pair)

    @pl.when(has_two)
    def _():
        for w in range(BACK - tiles - 1, -1, -1):
            hand(w).wait_recv()

            @pl.loop(0, w + 1)
            def _(i):
                @pl.when(i != far)
                def _():
                    all_pairs(i, w)

    bottom = jnp.maximum(far, jnp.maximum(BACK - tiles * plane, 0))
    for pair in range(pairs - 1):
        query_got(last, pair)

        @pl.loop(bottom, far + BACK + 1)
        def _(w):
            work(far, w, pair)

    def rest(w, late):
        if late:
            @pl.when(far <= w)
            def _():
                work(far, w, pairs - 1)
                if w < tiles:
                    put(w)
        elif w < last:
            @pl.when(far > w)
            def _():
                put(w)

    def carry(late):
        @pl.when(has_two)
        def _():
            for w in range(BACK - tiles):
                rest(w, late)

        @pl.when(has_down)
        def _():
            for w in range(BACK - tiles, BACK):
                rest(w, late)

    carry(False)
    for j in range(last):
        fill(flip(own, j))
    query_got(last, pairs - 1)
    for j in range(1, last):
        for pair in range(pairs):
            leave_start(pair, flip(own, j))
    carry(True)
    for pair in range(pairs):
        leave_start(pair, own)

    @pl.loop(0, far + 1)
    def _(t):
        work(far, t + BACK, pairs - 1)

    fill(far)
    for pair in range(pairs):
        leave_start(pair, far)

    @pl.when(has_down)
    def _():
        for w in range(tiles, BACK):
            @pl.when(has_up)
            def _():
                join(w)

            put(w)

    for w in range(BACK, window):
        @pl.when(has_up)
        def _():
            join(w)

        t = w - BACK
        dks[t * tile : (t + 1) * tile, :] = (acck[w] * scale).astype(bf16)
        dvs[t * tile : (t + 1) * tile, :] = accv[w].astype(bf16)
        leave_start(pairs, t)
        leave_start(pairs + 1, t)

    for which in range(leaves):
        leave_own(which).wait()
        for by in range(1, size):
            leave_got(which, by)
            leave_copy(which, flip(p, by)).wait_send()
    for kind in range(kinds):
        for by in range(1, size):
            entry_copy(kind, flip(p, by)).wait_send()
    for w in range(BACK):
        low = w < BACK - tiles

        @pl.when(has_up & has_down if low else has_up)
        def _():
            hand(w).wait_send()

        @pl.when(has_two if low else has_down)
        def _():
            back(w).wait_send()


def move(*refs):
    count = (len(refs) - 2) // 3
    ins, outs, held = refs[:count], refs[count : 2 * count], refs[2 * count : 3 * count]
    in_sem, out_sem = refs[3 * count :]
    reads = [pltpu.make_async_copy(a, b, in_sem.at[at]) for at, (a, b) in enumerate(zip(ins, held))]
    writes = [pltpu.make_async_copy(a, b, out_sem.at[at]) for at, (a, b) in enumerate(zip(held, outs))]
    for read in reads:
        read.start()
    for read, write in zip(reads, writes):
        read.wait()
        write.start()
    for write in writes:
        write.wait()


def shards(query, key, value, out, output_gradient, log_sum_exp, segment_ids):
    n, seqs = lax.axis_size("head"), lax.axis_size("seq")
    hd = HEAD_SIZE
    rows = query.shape[0]
    size = 2 * n
    cols = query.shape[1] // size
    width = cols // hd
    pairs = width // 2
    tile, tiles = 2 * rows, size // 2
    window = tiles + BACK
    bf16, f32 = jnp.bfloat16, jnp.float32
    kinds, leaves = 3 + 2 * pairs, pairs + 2
    vmem = pl.BlockSpec(memory_space=pltpu.VMEM)
    dma = pltpu.SemaphoreType.DMA
    anywhere = pl.BlockSpec(memory_space=pl.ANY)
    parts = pl.pallas_call(
        functools.partial(kernel, n, seqs, width),
        out_shape=[
            jax.ShapeDtypeStruct(query.shape, bf16),
            jax.ShapeDtypeStruct(key.shape, bf16),
            jax.ShapeDtypeStruct(value.shape, bf16),
        ],
        in_specs=[anywhere] * 5 + [vmem] * 2,
        out_specs=[anywhere] * 3,
        scratch_shapes=[
            pltpu.VMEM(key.shape, bf16),
            pltpu.VMEM(value.shape, bf16),
            pltpu.VMEM(query.shape, bf16),
            pltpu.VMEM(query.shape, bf16),
            pltpu.VMEM(query.shape, bf16),
            dma((5,)),
            pltpu.VMEM((size * rows, cols), bf16),
            pltpu.VMEM((size * rows, cols), bf16),
            pltpu.VMEM((size, 2 * width, rows), f32),
            pltpu.VMEM((2 * width, size * rows), f32),
            pltpu.VMEM((window, 2, tile, hd), bf16),
            pltpu.VMEM((window * tile, hd), f32),
            pltpu.VMEM((1, size * rows), f32),
            pltpu.VMEM((tiles, width, hd, tile), f32),
            pltpu.VMEM((window, tile, hd), f32),
            pltpu.VMEM((window, tile, hd), f32),
            pltpu.VMEM((BACK, 2, tile, hd), bf16),
            pltpu.VMEM((BACK, 2, tile, hd), bf16),
            pltpu.VMEM((size * rows, cols), bf16),
            pltpu.VMEM((size * rows, hd), bf16),
            pltpu.VMEM((size * rows, hd), bf16),
            dma((kinds + leaves,)),
            dma((kinds, size)),
            dma((kinds, size)),
            dma((BACK,)),
            dma((BACK,)),
            dma((BACK,)),
            dma((BACK,)),
            dma((leaves, size)),
            dma((leaves, size)),
        ],
        compiler_params=pltpu.CompilerParams(collective_id=0, has_side_effects=True),
    )(query, output_gradient, out, key, value, log_sum_exp.T, segment_ids.reshape(-1, hd))
    return pl.pallas_call(
        move,
        out_shape=[jax.ShapeDtypeStruct(part.shape, bf16) for part in parts],
        in_specs=[anywhere] * 3,
        out_specs=[anywhere] * 3,
        scratch_shapes=[pltpu.VMEM(part.shape, bf16) for part in parts] + [dma((3,)), dma((3,))],
    )(*parts)


def solution(mesh):
    placed = (P(("seq", "head"), None),) * 6 + (P(),)
    return jax.shard_map(
        lambda *a: tuple(shards(*a)),
        mesh=mesh,
        in_specs=placed,
        out_specs=(P(("seq", "head"), None),) * 3,
        check_vma=False,
    )
```

```python
import functools
import math

import jax
import jax.numpy as jnp
from jax import lax
from jax.experimental import pallas as pl
from jax.experimental.pallas import tpu as pltpu
from jax.sharding import PartitionSpec as P

HEAD_SIZE = 128
BACK = 6
LOG2E = math.log2(math.e)
MESH = pl.DeviceIdType.MESH
NT = (((1,), (1,)), ((), ()))


def dot(a, b):
    return jnp.dot(a, b, preferred_element_type=jnp.float32)


def dot_nt(a, b):
    return lax.dot_general(a, b, NT, preferred_element_type=jnp.float32)


def kernel(
    n, seqs, width,
    q_in, e_in, o_in, k_in, v_in, lse_ref, seg_ref,
    dq_out, dk_out, dv_out,
    k_ref, v_ref, e_ref, o_ref, q_ref, load_sem, qb, eb, stl, stb, kvb, segk, segq, dqt, acck, accv, ps, pr, dqs, dks, dvs,
    loc_sem, in_s, in_r, fw_s, fw_r, pt_s, pt_r, out_s, out_r,
):
    s = lax.axis_index("seq")
    h = lax.axis_index("head")
    rows = q_ref.shape[0]
    hd = HEAD_SIZE
    loads = [
        pltpu.make_async_copy(src, dst, load_sem.at[at])
        for at, (src, dst) in enumerate(((k_in, k_ref), (v_in, v_ref), (e_in, e_ref), (o_in, o_ref), (q_in, q_ref)))
    ]
    for load in loads:
        load.start()
    tile = 2 * rows
    size = 2 * n
    tiles = size // 2
    window = tiles + BACK
    cols = width * hd
    pairs = width // 2
    pcols = cols // pairs
    scale = 1.0 / math.sqrt(hd)
    f32, bf16 = jnp.float32, jnp.bfloat16

    def at(index, length):
        return pl.ds(index * length if isinstance(index, int) else pl.multiple_of(index * length, length), length)

    plane = s // 2
    p = lax.rem(s, 2) * n + h
    own = p // 2
    has_up, has_down, has_two = s + 2 < seqs, s >= 2, s >= 4

    def dev(index):
        return {"seq": s - lax.rem(s, 2) + index // n, "head": lax.rem(index, n)}

    def flip(value, by):
        bit = 1
        while bit <= by:
            if (by // bit) % 2:
                value = value + bit - 2 * bit * lax.rem(value // bit, 2)
            bit *= 2
        return value

    barrier = pltpu.get_barrier_semaphore()
    for by in range(1, size):
        pl.semaphore_signal(barrier, inc=1, device_id=dev(flip(p, by)), device_id_type=MESH)

    @pl.when(has_up)
    def _():
        pl.semaphore_signal(barrier, inc=1, device_id={"seq": s + 2}, device_id_type=MESH)

    @pl.when(has_down)
    def _():
        pl.semaphore_signal(barrier, inc=1, device_id={"seq": s - 2}, device_id_type=MESH)

    pl.semaphore_wait(barrier, size - 1 + jnp.minimum(s // 2, 1) + jnp.minimum((seqs - 1 - s) // 2, 1))

    kinds = 3 + 2 * pairs

    def entry(kind, to, me):
        if kind < 2:
            dst = kvb.at[BACK + me // 2, kind, at(lax.rem(me, 2), rows), :]
            return (k_ref, v_ref)[kind].at[:, at(to, hd)], dst
        if kind == 2:
            return stl.at[to], stb.at[:, at(me, rows)]
        pair, which = (kind - 3) // 2, (kind - 3) % 2
        src = (q_ref, e_ref)[which].at[:, at(to * pairs + pair, pcols)]
        return src, (qb, eb)[which].at[at(me, rows), pl.ds(pair * pcols, pcols)]

    def entry_copy(kind, to):
        src, dst = entry(kind, to, p)
        return pltpu.make_async_remote_copy(
            src_ref=src, dst_ref=dst, send_sem=in_s.at[kind, to], recv_sem=in_r.at[kind, p],
            device_id=dev(to), device_id_type=MESH)

    def entry_got(kind, by):
        _, dst = entry(kind, p, flip(p, by))
        pltpu.make_async_remote_copy(
            src_ref=dst, dst_ref=dst, send_sem=in_s.at[kind, flip(p, by)], recv_sem=in_r.at[kind, flip(p, by)],
            device_id=dev(flip(p, by)), device_id_type=MESH).wait_recv()

    def entry_own(kind):
        src, dst = entry(kind, p, p)
        return pltpu.make_async_copy(src, dst, loc_sem.at[kind])

    order = tuple(sorted(range(1, size), key=lambda by: (by // 2 > 0, by // 2 == 3, by % 2, by)))

    for kind in (0, 1):
        loads[kind].wait()
        entry_own(kind).start()
    for by in order:
        for kind in (0, 1):
            entry_copy(kind, flip(p, by)).start()
    loads[2].wait()
    loads[3].wait()

    lane = lax.broadcasted_iota(jnp.int32, (rows, hd), 1)
    delta = jnp.zeros((rows, hd), f32)
    for head in range(width * size):
        here = pl.ds(head * hd, hd)
        one = jnp.sum(e_ref[:, here].astype(f32) * o_ref[:, here].astype(f32), axis=1, keepdims=True)
        delta = jnp.where(lane == head, one, delta)
    delta = delta.T
    for to in range(size):
        stl[to, :width, :] = lse_ref[to * width : (to + 1) * width, :] * LOG2E
        stl[to, width:, :] = delta[to * width : (to + 1) * width, :]
    entry_own(2).start()
    for by in order:
        entry_copy(2, flip(p, by)).start()
    loads[4].wait()
    for kind in range(3, kinds):
        entry_own(kind).start()
        entry_copy(kind, flip(p, 1)).start()
    for near in (order[1:5], order[5:]):
        for kind in range(3, kinds):
            for by in near:
                entry_copy(kind, flip(p, by)).start()

    first = plane * size - BACK * 2
    for a in range(2 * window):
        row = seg_ref[pl.ds(jnp.maximum(first + a, 0), 1), :].astype(f32)
        segk[a * rows : (a + 1) * rows, :] = jnp.broadcast_to(row, (rows, hd)).T
        if a >= 2 * BACK:
            segq[:, (a - 2 * BACK) * rows : (a - 2 * BACK + 1) * rows] = row
    dqt[...] = jnp.zeros_like(dqt)
    acck[...] = jnp.zeros_like(acck)
    accv[...] = jnp.zeros_like(accv)

    def hand(w):
        return pltpu.make_async_remote_copy(
            src_ref=kvb.at[w + tiles], dst_ref=kvb.at[w], send_sem=fw_s.at[w], recv_sem=fw_r.at[w],
            device_id={"seq": s + 2}, device_id_type=MESH)

    def back(w):
        return pltpu.make_async_remote_copy(
            src_ref=ps.at[w], dst_ref=pr.at[w], send_sem=pt_s.at[w], recv_sem=pt_r.at[w],
            device_id={"seq": s - 2}, device_id_type=MESH)

    row_at = lax.broadcasted_iota(jnp.int32, (tile, tile), 0)
    col_at = lax.broadcasted_iota(jnp.int32, (tile, tile), 1)

    def work(i, w, pair):
        q_rows = at(i, tile)
        key, val = kvb[w, 0], kvb[w, 1]
        key_t = key.T
        k_seg = segk[at(w, tile), :]
        allowed = jnp.concatenate([k_seg] * (tile // hd), axis=1) == segq[:, q_rows]
        if not isinstance(w, int) or w >= BACK:
            allowed &= row_at + (w - BACK - i) * tile <= col_at
        mine = range(pair * width // pairs, (pair + 1) * width // pairs)
        queries = [qb[q_rows, m * hd : (m + 1) * hd] for m in mine]
        grads = [eb[q_rows, m * hd : (m + 1) * hd] for m in mine]
        scores = [dot_nt(key, query) for query in queries]
        dprobs = [dot_nt(val, grad) for grad in grads]
        low, dscores = [], []
        for m, score, dprob in zip(mine, scores, dprobs):
            lse = stb[m : m + 1, q_rows]
            delta = stb[width + m : width + m + 1, q_rows]
            probs = jnp.exp2(jnp.where(allowed, score * (scale * LOG2E) - lse, -jnp.inf))
            low.append(probs.astype(bf16))
            dscores.append((probs * (dprob - delta)).astype(bf16))
        accv[w] += dot(jnp.concatenate(low, axis=1), jnp.concatenate(grads, axis=0))
        acck[w] += dot(jnp.concatenate(dscores, axis=1), jnp.concatenate(queries, axis=0))
        for m, dscore in zip(mine, dscores):
            dqt[i, m] += dot(key_t, dscore)

    def leave(which, to, me):
        if which < pairs:
            src = dqs.at[at(to, rows), pl.ds(which * pcols, pcols)]
            return src, dq_out.at[:, at(me * pairs + which, pcols)]
        src, dst = ((dks, dk_out), (dvs, dv_out))[which - pairs]
        return src.at[at(to, rows), :], dst.at[:, at(me, hd)]

    leaves = pairs + 2

    def leave_copy(which, to):
        src, dst = leave(which, to, p)
        return pltpu.make_async_remote_copy(
            src_ref=src, dst_ref=dst, send_sem=out_s.at[which, to], recv_sem=out_r.at[which, p],
            device_id=dev(to), device_id_type=MESH)

    def leave_got(which, by):
        _, dst = leave(which, p, flip(p, by))
        pltpu.make_async_remote_copy(
            src_ref=dst, dst_ref=dst, send_sem=out_s.at[which, flip(p, by)], recv_sem=out_r.at[which, flip(p, by)],
            device_id=dev(flip(p, by)), device_id_type=MESH).wait_recv()

    def leave_own(which):
        src, dst = leave(which, p, p)
        return pltpu.make_async_copy(src, dst, loc_sem.at[kinds + which])

    def leave_start(which, i):
        for b in range(2):
            to = 2 * i + b

            @pl.when(to != p)
            def _():
                leave_copy(which, to).start()

            @pl.when(to == p)
            def _():
                leave_own(which).start()

    def fill(i):
        for m in range(width):
            dqs[at(i, tile), m * hd : (m + 1) * hd] = (dqt[i, m] * scale).T.astype(bf16)

    def by_twos(i, start, stop, pair):
        count = stop - start

        @pl.loop(0, count // 2)
        def _(t):
            work(i, start + 2 * t, pair)
            work(i, start + 2 * t + 1, pair)

        @pl.when(lax.rem(count, 2) == 1)
        def _():
            work(i, stop - 1, pair)

    def all_pairs(i, w):
        for pair in range(pairs):
            work(i, w, pair)

    def query_got(j, pair):
        for by in range(2 * j, 2 * j + 2):
            for kind in ((2,) if pair == 0 else ()) + (3 + 2 * pair, 4 + 2 * pair):
                entry_got(kind, by)

    def put(w):
        ps[w, 0] = acck[w].astype(bf16)
        ps[w, 1] = accv[w].astype(bf16)
        back(w).start()

    def join(w):
        back(w - tiles).wait_recv()
        acck[w] += pr[w - tiles, 0].astype(f32)
        accv[w] += pr[w - tiles, 1].astype(f32)

    for kind in range(kinds):
        entry_own(kind).wait()
    for j in range(tiles):
        for by in range(max(2 * j, 1), 2 * j + 2):
            entry_got(0, by)
            entry_got(1, by)
        t = flip(own, j)

        @pl.when(has_up)
        def _():
            hand(t + BACK - tiles).start()

        if j == 0:
            for kind in range(2, kinds):
                entry_got(kind, 1)

        @pl.when(t <= own)
        def _():
            all_pairs(own, t + BACK)

    last = tiles - 1
    far = flip(own, last)

    def before(j):
        w = BACK - tiles + flip(own, j)

        @pl.when(has_down)
        def _():
            hand(w).wait_recv()

            @pl.when(has_up & (w >= tiles))
            def _():
                hand(w - tiles).start()

            @pl.when(own <= w)
            def _():
                all_pairs(own, w)

    sides = [flip(own, j) for j in range(1, last)]

    def near(w, pair):
        for i in sides:
            if w >= tiles - 1:
                work(i, w, pair)
            else:
                @pl.when(i <= w)
                def _():
                    work(i, w, pair)

    for j in range(last):
        before(j)
    for pair in range(pairs):
        for j in range(1, last):
            query_got(j, pair)
            i = flip(own, j)
            by_twos(i, BACK, i + BACK + 1, pair)

        if pair == 0:
            before(last)

        @pl.when(has_down)
        def _():
            for w in range(BACK - tiles, BACK):
                near(w, pair)

    @pl.when(has_two)
    def _():
        for w in range(BACK - tiles - 1, -1, -1):
            hand(w).wait_recv()

            @pl.loop(0, w + 1)
            def _(i):
                @pl.when(i != far)
                def _():
                    all_pairs(i, w)

    for j in range(last):
        fill(flip(own, j))

    for w in range(last):
        @pl.when((has_two if w < BACK - tiles else has_down) & (far > w))
        def _():
            put(w)

    bottom = jnp.maximum(far, jnp.maximum(BACK - tiles * plane, 0))
    for pair in range(pairs - 1):
        query_got(last, pair)
        by_twos(far, bottom, far + BACK + 1, pair)
    query_got(last, pairs - 1)
    for j in range(1, last):
        for pair in range(pairs):
            leave_start(pair, flip(own, j))

    def rest(*some):
        for w in some:
            work(far, w, pairs - 1)
        for w in some:
            @pl.when(w < tiles)
            def _():
                put(w)

    @pl.when(has_two)
    def _():
        for w in range(0, BACK - tiles, 2):
            @pl.when(far <= w)
            def _():
                rest(w, w + 1)

            @pl.when(far == w + 1)
            def _():
                rest(w + 1)

    turns = tuple(range(tiles - 1, -1, -1))
    ws = [BACK - tiles + flip(own, j) for j in turns]

    @pl.when(has_down)
    def _():
        rest(*ws[:2])

        @pl.when(far <= ws[3])
        def _():
            rest(*ws[2:])

        @pl.when(far > ws[3])
        def _():
            rest(ws[2])

    for pair in range(pairs):
        leave_start(pair, own)
    by_twos(far, BACK, far + BACK + 1, pairs - 1)
    fill(far)
    for pair in range(pairs):
        leave_start(pair, far)

    @pl.when(has_down)
    def _():
        for w in ws:
            @pl.when(w >= tiles)
            def _():
                @pl.when(has_up)
                def _():
                    join(w)

                put(w)

    for j in turns:
        t = flip(own, j)
        w = t + BACK

        @pl.when(has_up)
        def _():
            join(w)

        dks[at(t, tile), :] = (acck[w] * scale).astype(bf16)
        dvs[at(t, tile), :] = accv[w].astype(bf16)
        leave_start(pairs, t)
        leave_start(pairs + 1, t)

    for which in range(leaves):
        leave_own(which).wait()
        for by in range(1, size):
            leave_got(which, by)
            leave_copy(which, flip(p, by)).wait_send()
    for kind in range(kinds):
        for by in range(1, size):
            entry_copy(kind, flip(p, by)).wait_send()
    for w in range(BACK):
        low = w < BACK - tiles

        @pl.when(has_up & has_down if low else has_up)
        def _():
            hand(w).wait_send()

        @pl.when(has_two if low else has_down)
        def _():
            back(w).wait_send()


def move(*refs):
    ins, outs, sems = refs[:3], refs[3:6], refs[6]
    copies = [pltpu.make_async_copy(a, b, sems.at[at]) for at, (a, b) in enumerate(zip(ins, outs))]
    for copy in copies:
        copy.start()
    for copy in copies:
        copy.wait()


def shards(query, key, value, out, output_gradient, log_sum_exp, segment_ids):
    n, seqs = lax.axis_size("head"), lax.axis_size("seq")
    hd = HEAD_SIZE
    rows = query.shape[0]
    size = 2 * n
    cols = query.shape[1] // size
    width = cols // hd
    pairs = width // 2
    tile, tiles = 2 * rows, size // 2
    window = tiles + BACK
    bf16, f32 = jnp.bfloat16, jnp.float32
    kinds, leaves = 3 + 2 * pairs, pairs + 2
    vmem = pl.BlockSpec(memory_space=pltpu.VMEM)
    dma = pltpu.SemaphoreType.DMA
    anywhere = pl.BlockSpec(memory_space=pl.ANY)
    parts = pl.pallas_call(
        functools.partial(kernel, n, seqs, width),
        out_shape=[pltpu.VMEM(like.shape, bf16) for like in (query, key, value)],
        in_specs=[anywhere] * 5 + [vmem] * 2,
        out_specs=[vmem] * 3,
        scratch_shapes=[
            pltpu.VMEM(key.shape, bf16),
            pltpu.VMEM(value.shape, bf16),
            pltpu.VMEM(query.shape, bf16),
            pltpu.VMEM(query.shape, bf16),
            pltpu.VMEM(query.shape, bf16),
            dma((5,)),
            pltpu.VMEM((size * rows, cols), bf16),
            pltpu.VMEM((size * rows, cols), bf16),
            pltpu.VMEM((size, 2 * width, rows), f32),
            pltpu.VMEM((2 * width, size * rows), f32),
            pltpu.VMEM((window, 2, tile, hd), bf16),
            pltpu.VMEM((window * tile, hd), f32),
            pltpu.VMEM((1, size * rows), f32),
            pltpu.VMEM((tiles, width, hd, tile), f32),
            pltpu.VMEM((window, tile, hd), f32),
            pltpu.VMEM((window, tile, hd), f32),
            pltpu.VMEM((BACK, 2, tile, hd), bf16),
            pltpu.VMEM((BACK, 2, tile, hd), bf16),
            pltpu.VMEM((size * rows, cols), bf16),
            pltpu.VMEM((size * rows, hd), bf16),
            pltpu.VMEM((size * rows, hd), bf16),
            dma((kinds + leaves,)),
            dma((kinds, size)),
            dma((kinds, size)),
            dma((BACK,)),
            dma((BACK,)),
            dma((BACK,)),
            dma((BACK,)),
            dma((leaves, size)),
            dma((leaves, size)),
        ],
        compiler_params=pltpu.CompilerParams(collective_id=0, has_side_effects=True),
    )(query, output_gradient, out, key, value, log_sum_exp.T, segment_ids.reshape(-1, hd))
    return pl.pallas_call(
        move,
        out_shape=[jax.ShapeDtypeStruct(part.shape, bf16) for part in parts],
        in_specs=[vmem] * 3,
        out_specs=[anywhere] * 3,
        scratch_shapes=[dma((3,))],
        compiler_params=pltpu.CompilerParams(vmem_limit_bytes=1 << 20),
    )(*parts)


def solution(mesh):
    placed = (P(("seq", "head"), None),) * 6 + (P(),)
    return jax.shard_map(
        lambda *a: tuple(shards(*a)),
        mesh=mesh,
        in_specs=placed,
        out_specs=(P(("seq", "head"), None),) * 3,
        check_vma=False,
    )
```

```python
import functools
import math

import jax
import jax.numpy as jnp
from jax import lax
from jax.experimental import pallas as pl
from jax.experimental.pallas import tpu as pltpu
from jax.sharding import PartitionSpec as P

HEAD_SIZE = 128
BACK = 6
LOG2E = math.log2(math.e)
MESH = pl.DeviceIdType.MESH
NT = (((1,), (1,)), ((), ()))


def dot(a, b):
    return jnp.dot(a, b, preferred_element_type=jnp.float32)


def dot_nt(a, b):
    return lax.dot_general(a, b, NT, preferred_element_type=jnp.float32)


def kernel(
    n, seqs, width,
    q_in, e_in, o_in, k_in, v_in, lse_ref, seg_ref,
    dq_out, dk_out, dv_out,
    k_ref, v_ref, e_ref, o_ref, q_ref, load_sem, qb, eb, stl, stb, kvb, segk, segq, dqt, acck, accv, ps, pr, dqs, dks, dvs,
    loc_sem, in_s, in_r, fw_s, fw_r, pt_s, pt_r, out_s, out_r,
):
    s = lax.axis_index("seq")
    h = lax.axis_index("head")
    rows = q_ref.shape[0]
    hd = HEAD_SIZE
    loads = [
        pltpu.make_async_copy(src, dst, load_sem.at[at])
        for at, (src, dst) in enumerate(((k_in, k_ref), (v_in, v_ref), (e_in, e_ref), (o_in, o_ref), (q_in, q_ref)))
    ]
    for load in loads:
        load.start()
    tile = 2 * rows
    size = 2 * n
    tiles = size // 2
    window = tiles + BACK
    cols = width * hd
    pairs = width // 2
    pcols = cols // pairs
    scale = 1.0 / math.sqrt(hd)
    f32, bf16 = jnp.float32, jnp.bfloat16

    def at(index, length):
        return pl.ds(index * length if isinstance(index, int) else pl.multiple_of(index * length, length), length)

    plane = s // 2
    p = lax.rem(s, 2) * n + h
    own = p // 2
    has_up, has_down, has_two = s + 2 < seqs, s >= 2, s >= 4

    def dev(index):
        return {"seq": s - lax.rem(s, 2) + index // n, "head": lax.rem(index, n)}

    def flip(value, by):
        bit = 1
        while bit <= by:
            if (by // bit) % 2:
                value = value + bit - 2 * bit * lax.rem(value // bit, 2)
            bit *= 2
        return value

    barrier = pltpu.get_barrier_semaphore()
    for by in range(1, size):
        pl.semaphore_signal(barrier, inc=1, device_id=dev(flip(p, by)), device_id_type=MESH)

    @pl.when(has_up)
    def _():
        pl.semaphore_signal(barrier, inc=1, device_id={"seq": s + 2}, device_id_type=MESH)

    @pl.when(has_down)
    def _():
        pl.semaphore_signal(barrier, inc=1, device_id={"seq": s - 2}, device_id_type=MESH)

    pl.semaphore_wait(barrier, size - 1 + jnp.minimum(s // 2, 1) + jnp.minimum((seqs - 1 - s) // 2, 1))

    kinds = 3 + 2 * pairs

    def entry(kind, to, me):
        if kind < 2:
            dst = kvb.at[BACK + me // 2, kind, at(lax.rem(me, 2), rows), :]
            return (k_ref, v_ref)[kind].at[:, at(to, hd)], dst
        if kind == 2:
            return stl.at[to], stb.at[:, at(me, rows)]
        pair, which = (kind - 3) // 2, (kind - 3) % 2
        src = (q_ref, e_ref)[which].at[:, at(to * pairs + pair, pcols)]
        return src, (qb, eb)[which].at[at(me, rows), pl.ds(pair * pcols, pcols)]

    def entry_copy(kind, to):
        src, dst = entry(kind, to, p)
        return pltpu.make_async_remote_copy(
            src_ref=src, dst_ref=dst, send_sem=in_s.at[kind, to], recv_sem=in_r.at[kind, p],
            device_id=dev(to), device_id_type=MESH)

    def entry_got(kind, by):
        _, dst = entry(kind, p, flip(p, by))
        pltpu.make_async_remote_copy(
            src_ref=dst, dst_ref=dst, send_sem=in_s.at[kind, flip(p, by)], recv_sem=in_r.at[kind, flip(p, by)],
            device_id=dev(flip(p, by)), device_id_type=MESH).wait_recv()

    def entry_own(kind):
        src, dst = entry(kind, p, p)
        return pltpu.make_async_copy(src, dst, loc_sem.at[kind])

    order = tuple(sorted(range(1, size), key=lambda by: (by // 2 > 0, by // 2 == 3, by % 2, by)))

    for kind in (0, 1):
        loads[kind].wait()
        entry_own(kind).start()
    for by in order:
        for kind in (0, 1):
            entry_copy(kind, flip(p, by)).start()
    loads[2].wait()
    loads[3].wait()

    lane = lax.broadcasted_iota(jnp.int32, (rows, hd), 1)
    delta = jnp.zeros((rows, hd), f32)
    for head in range(width * size):
        here = pl.ds(head * hd, hd)
        one = jnp.sum(e_ref[:, here].astype(f32) * o_ref[:, here].astype(f32), axis=1, keepdims=True)
        delta = jnp.where(lane == head, one, delta)
    delta = delta.T
    for to in range(size):
        stl[to, :width, :] = lse_ref[to * width : (to + 1) * width, :] * LOG2E
        stl[to, width:, :] = delta[to * width : (to + 1) * width, :]
    entry_own(2).start()
    for by in order:
        entry_copy(2, flip(p, by)).start()
    loads[4].wait()
    for kind in range(3, kinds):
        entry_own(kind).start()
        entry_copy(kind, flip(p, 1)).start()
    def peer(base, core):
        chip = flip(p, base)
        return chip - lax.rem(chip, 2) + core

    for bases, core, pair in (
        ((2, 4), 1, 0),
        ((2, 4), 0, 0),
        ((2, 4), 1, 1),
        ((6,), 1, 0),
        ((2, 4), 0, 1),
        ((6,), 1, 1),
        ((6,), 0, 0),
        ((6,), 0, 1),
    ):
        for base in bases:
            for which in range(2):
                entry_copy(3 + 2 * pair + which, peer(base, core)).start()

    first = plane * size - BACK * 2
    for a in range(2 * window):
        row = seg_ref[pl.ds(jnp.maximum(first + a, 0), 1), :].astype(f32)
        segk[a * rows : (a + 1) * rows, :] = jnp.broadcast_to(row, (rows, hd)).T
        if a >= 2 * BACK:
            segq[:, (a - 2 * BACK) * rows : (a - 2 * BACK + 1) * rows] = row
    dqt[...] = jnp.zeros_like(dqt)
    acck[...] = jnp.zeros_like(acck)
    accv[...] = jnp.zeros_like(accv)

    def hand(w):
        return pltpu.make_async_remote_copy(
            src_ref=kvb.at[w + tiles], dst_ref=kvb.at[w], send_sem=fw_s.at[w], recv_sem=fw_r.at[w],
            device_id={"seq": s + 2}, device_id_type=MESH)

    def back(w):
        return pltpu.make_async_remote_copy(
            src_ref=ps.at[w], dst_ref=pr.at[w], send_sem=pt_s.at[w], recv_sem=pt_r.at[w],
            device_id={"seq": s - 2}, device_id_type=MESH)

    row_at = lax.broadcasted_iota(jnp.int32, (tile, tile), 0)
    col_at = lax.broadcasted_iota(jnp.int32, (tile, tile), 1)

    def work(i, w, pair):
        q_rows = at(i, tile)
        key, val = kvb[w, 0], kvb[w, 1]
        key_t = key.T
        k_seg = segk[at(w, tile), :]
        allowed = jnp.concatenate([k_seg] * (tile // hd), axis=1) == segq[:, q_rows]
        if not isinstance(w, int) or w >= BACK:
            allowed &= row_at + (w - BACK - i) * tile <= col_at
        mine = range(pair * width // pairs, (pair + 1) * width // pairs)
        queries = [qb[q_rows, m * hd : (m + 1) * hd] for m in mine]
        grads = [eb[q_rows, m * hd : (m + 1) * hd] for m in mine]
        scores = [dot_nt(key, query) for query in queries]
        dprobs = [dot_nt(val, grad) for grad in grads]
        low, dscores = [], []
        for m, score, dprob in zip(mine, scores, dprobs):
            lse = stb[m : m + 1, q_rows]
            delta = stb[width + m : width + m + 1, q_rows]
            probs = jnp.exp2(jnp.where(allowed, score * (scale * LOG2E) - lse, -jnp.inf))
            low.append(probs.astype(bf16))
            dscores.append((probs * (dprob - delta)).astype(bf16))
        accv[w] += dot(jnp.concatenate(low, axis=1), jnp.concatenate(grads, axis=0))
        acck[w] += dot(jnp.concatenate(dscores, axis=1), jnp.concatenate(queries, axis=0))
        for m, dscore in zip(mine, dscores):
            dqt[i, m] += dot(key_t, dscore)

    def leave(which, to, me):
        if which < pairs:
            src = dqs.at[at(to, rows), pl.ds(which * pcols, pcols)]
            return src, dq_out.at[:, at(me * pairs + which, pcols)]
        src, dst = ((dks, dk_out), (dvs, dv_out))[which - pairs]
        return src.at[at(to, rows), :], dst.at[:, at(me, hd)]

    leaves = pairs + 2

    def leave_copy(which, to):
        src, dst = leave(which, to, p)
        return pltpu.make_async_remote_copy(
            src_ref=src, dst_ref=dst, send_sem=out_s.at[which, to], recv_sem=out_r.at[which, p],
            device_id=dev(to), device_id_type=MESH)

    def leave_got(which, by):
        _, dst = leave(which, p, flip(p, by))
        pltpu.make_async_remote_copy(
            src_ref=dst, dst_ref=dst, send_sem=out_s.at[which, flip(p, by)], recv_sem=out_r.at[which, flip(p, by)],
            device_id=dev(flip(p, by)), device_id_type=MESH).wait_recv()

    def leave_own(which):
        src, dst = leave(which, p, p)
        return pltpu.make_async_copy(src, dst, loc_sem.at[kinds + which])

    def leave_start(which, i):
        for b in range(2):
            to = 2 * i + b

            @pl.when(to != p)
            def _():
                leave_copy(which, to).start()

            @pl.when(to == p)
            def _():
                leave_own(which).start()

    def fill(i, pair):
        for m in range(pair * width // pairs, (pair + 1) * width // pairs):
            dqs[at(i, tile), m * hd : (m + 1) * hd] = (dqt[i, m] * scale).T.astype(bf16)

    def by_twos(i, start, stop, pair):
        count = stop - start

        @pl.loop(0, count // 2)
        def _(t):
            work(i, start + 2 * t, pair)
            work(i, start + 2 * t + 1, pair)

        @pl.when(lax.rem(count, 2) == 1)
        def _():
            work(i, stop - 1, pair)

    def all_pairs(i, w):
        for pair in range(pairs):
            work(i, w, pair)

    def query_got(j, pair):
        for by in range(2 * j, 2 * j + 2):
            for kind in ((2,) if pair == 0 else ()) + (3 + 2 * pair, 4 + 2 * pair):
                entry_got(kind, by)

    def put(w):
        ps[w, 0] = acck[w].astype(bf16)
        ps[w, 1] = accv[w].astype(bf16)
        back(w).start()

    def join(w):
        back(w - tiles).wait_recv()
        acck[w] += pr[w - tiles, 0].astype(f32)
        accv[w] += pr[w - tiles, 1].astype(f32)

    for kind in range(kinds):
        entry_own(kind).wait()
    for j in range(tiles):
        for by in range(max(2 * j, 1), 2 * j + 2):
            entry_got(0, by)
            entry_got(1, by)
        t = flip(own, j)

        @pl.when(has_up)
        def _():
            hand(t + BACK - tiles).start()

        if j == 0:
            for kind in range(2, kinds):
                entry_got(kind, 1)

        @pl.when(t <= own)
        def _():
            all_pairs(own, t + BACK)

    last = tiles - 1
    far = flip(own, last)

    def before(j):
        w = BACK - tiles + flip(own, j)

        @pl.when(has_down)
        def _():
            hand(w).wait_recv()

            @pl.when(has_up & (w >= tiles))
            def _():
                hand(w - tiles).start()

            @pl.when(own <= w)
            def _():
                all_pairs(own, w)

    sides = [flip(own, j) for j in range(1, last)]

    def near(w, pair):
        for i in sides:
            if w >= tiles - 1:
                work(i, w, pair)
            else:
                @pl.when(i <= w)
                def _():
                    work(i, w, pair)

    for j in range(last):
        before(j)
    for pair in range(pairs):
        for j in range(1, last):
            query_got(j, pair)
            i = flip(own, j)
            if pair == 0:
                by_twos(i, BACK, i + BACK + 1, pair)

        if pair == 0:
            before(last)

        @pl.when(has_down)
        def _():
            for w in range(BACK - tiles, BACK):
                near(w, pair)

    @pl.when(has_two)
    def _():
        for w in range(BACK - tiles - 1, -1, -1):
            hand(w).wait_recv()

            @pl.loop(0, w + 1)
            def _(i):
                @pl.when(i != far)
                def _():
                    all_pairs(i, w)

    for pair in range(pairs):
        fill(own, pair)
    for i in sides:
        fill(i, 0)

    for w in range(last):
        @pl.when((has_two if w < BACK - tiles else has_down) & (far > w))
        def _():
            put(w)

    bottom = jnp.maximum(far, jnp.maximum(BACK - tiles * plane, 0))
    for pair in range(pairs - 1):
        query_got(last, pair)
        by_twos(far, jnp.minimum(bottom, BACK), BACK, pair)
    query_got(last, pairs - 1)
    for i in sides:
        leave_start(0, i)

    def rest(*some):
        for w in some:
            work(far, w, pairs - 1)
        for w in some:
            @pl.when(w < tiles)
            def _():
                put(w)

    @pl.when(has_two)
    def _():
        for w in range(0, BACK - tiles, 2):
            @pl.when(far <= w)
            def _():
                rest(w, w + 1)

            @pl.when(far == w + 1)
            def _():
                rest(w + 1)

    turns = tuple(range(tiles - 1, -1, -1))
    ws = [BACK - tiles + flip(own, j) for j in turns]

    @pl.when(has_down)
    def _():
        rest(*ws[:2])

        @pl.when(far <= ws[3])
        def _():
            rest(*ws[2:])

        @pl.when(far > ws[3])
        def _():
            rest(ws[2])

    for pair in range(pairs):
        leave_start(pair, own)
    for i in sides:
        for pair in range(1, pairs):
            by_twos(i, BACK, i + BACK + 1, pair)
            fill(i, pair)
            leave_start(pair, i)

    @pl.loop(BACK, far + BACK + 1)
    def _(w):
        all_pairs(far, w)

    for pair in range(pairs):
        fill(far, pair)
        leave_start(pair, far)

    @pl.when(has_down)
    def _():
        for w in ws:
            @pl.when(w >= tiles)
            def _():
                @pl.when(has_up)
                def _():
                    join(w)

                put(w)

    for j in turns:
        t = flip(own, j)
        w = t + BACK

        @pl.when(has_up)
        def _():
            join(w)

        dks[at(t, tile), :] = (acck[w] * scale).astype(bf16)
        dvs[at(t, tile), :] = accv[w].astype(bf16)
        leave_start(pairs, t)
        leave_start(pairs + 1, t)

    for which in range(leaves):
        leave_own(which).wait()
        for by in range(1, size):
            leave_got(which, by)
            leave_copy(which, flip(p, by)).wait_send()
    for kind in range(kinds):
        for by in range(1, size):
            entry_copy(kind, flip(p, by)).wait_send()
    for w in range(BACK):
        low = w < BACK - tiles

        @pl.when(has_up & has_down if low else has_up)
        def _():
            hand(w).wait_send()

        @pl.when(has_two if low else has_down)
        def _():
            back(w).wait_send()


def move(*refs):
    ins, outs, sems = refs[:3], refs[3:6], refs[6]
    copies = [pltpu.make_async_copy(a, b, sems.at[at]) for at, (a, b) in enumerate(zip(ins, outs))]
    for copy in copies:
        copy.start()
    for copy in copies:
        copy.wait()


def shards(query, key, value, out, output_gradient, log_sum_exp, segment_ids):
    n, seqs = lax.axis_size("head"), lax.axis_size("seq")
    hd = HEAD_SIZE
    rows = query.shape[0]
    size = 2 * n
    cols = query.shape[1] // size
    width = cols // hd
    pairs = width // 2
    tile, tiles = 2 * rows, size // 2
    window = tiles + BACK
    bf16, f32 = jnp.bfloat16, jnp.float32
    kinds, leaves = 3 + 2 * pairs, pairs + 2
    vmem = pl.BlockSpec(memory_space=pltpu.VMEM)
    dma = pltpu.SemaphoreType.DMA
    anywhere = pl.BlockSpec(memory_space=pl.ANY)
    parts = pl.pallas_call(
        functools.partial(kernel, n, seqs, width),
        out_shape=[pltpu.VMEM(like.shape, bf16) for like in (query, key, value)],
        in_specs=[anywhere] * 5 + [vmem] * 2,
        out_specs=[vmem] * 3,
        scratch_shapes=[
            pltpu.VMEM(key.shape, bf16),
            pltpu.VMEM(value.shape, bf16),
            pltpu.VMEM(query.shape, bf16),
            pltpu.VMEM(query.shape, bf16),
            pltpu.VMEM(query.shape, bf16),
            dma((5,)),
            pltpu.VMEM((size * rows, cols), bf16),
            pltpu.VMEM((size * rows, cols), bf16),
            pltpu.VMEM((size, 2 * width, rows), f32),
            pltpu.VMEM((2 * width, size * rows), f32),
            pltpu.VMEM((window, 2, tile, hd), bf16),
            pltpu.VMEM((window * tile, hd), f32),
            pltpu.VMEM((1, size * rows), f32),
            pltpu.VMEM((tiles, width, hd, tile), f32),
            pltpu.VMEM((window, tile, hd), f32),
            pltpu.VMEM((window, tile, hd), f32),
            pltpu.VMEM((BACK, 2, tile, hd), bf16),
            pltpu.VMEM((BACK, 2, tile, hd), bf16),
            pltpu.VMEM((size * rows, cols), bf16),
            pltpu.VMEM((size * rows, hd), bf16),
            pltpu.VMEM((size * rows, hd), bf16),
            dma((kinds + leaves,)),
            dma((kinds, size)),
            dma((kinds, size)),
            dma((BACK,)),
            dma((BACK,)),
            dma((BACK,)),
            dma((BACK,)),
            dma((leaves, size)),
            dma((leaves, size)),
        ],
        compiler_params=pltpu.CompilerParams(collective_id=0, has_side_effects=True),
    )(query, output_gradient, out, key, value, log_sum_exp.T, segment_ids.reshape(-1, hd))
    return pl.pallas_call(
        move,
        out_shape=[jax.ShapeDtypeStruct(part.shape, bf16) for part in parts],
        in_specs=[vmem] * 3,
        out_specs=[anywhere] * 3,
        scratch_shapes=[dma((3,))],
        compiler_params=pltpu.CompilerParams(vmem_limit_bytes=1 << 20),
    )(*parts)


def solution(mesh):
    placed = (P(("seq", "head"), None),) * 6 + (P(),)
    return jax.shard_map(
        lambda *a: tuple(shards(*a)),
        mesh=mesh,
        in_specs=placed,
        out_specs=(P(("seq", "head"), None),) * 3,
        check_vma=False,
    )
```

```python
import functools
import math

import jax
import jax.numpy as jnp
from jax import lax
from jax.experimental import pallas as pl
from jax.experimental.pallas import tpu as pltpu
from jax.sharding import PartitionSpec as P

HEAD_SIZE = 128
BACK = 6
LOG2E = math.log2(math.e)
MESH = pl.DeviceIdType.MESH
NT = (((1,), (1,)), ((), ()))


def dot(a, b):
    return jnp.dot(a, b, preferred_element_type=jnp.float32)


def dot_nt(a, b):
    return lax.dot_general(a, b, NT, preferred_element_type=jnp.float32)


def kernel(
    n, seqs, width,
    q_in, e_in, o_in, k_in, v_in, lse_in, seg_in,
    dq_out, dk_out, dv_out,
    k_ref, v_ref, e_ref, o_ref, q_ref, lse_ref, seg_ref, load_sem, qb, eb, stl, stb, kvb, segk, segq, dqt, acck, accv, ps, pr, dqs, dks, dvs,
    loc_sem, in_s, in_r, fw_s, fw_r, pt_s, pt_r, out_s, out_r,
):
    s = lax.axis_index("seq")
    h = lax.axis_index("head")
    rows = q_ref.shape[0]
    hd = HEAD_SIZE
    loads = [
        pltpu.make_async_copy(src, dst, load_sem.at[at])
        for at, (src, dst) in enumerate((
            (k_in, k_ref), (v_in, v_ref), (e_in, e_ref), (o_in, o_ref), (q_in, q_ref), (lse_in, lse_ref), (seg_in, seg_ref),
        ))
    ]
    for load in loads:
        load.start()
    tile = 2 * rows
    size = 2 * n
    tiles = size // 2
    window = tiles + BACK
    cols = width * hd
    pairs = width // 2
    pcols = cols // pairs
    scale = 1.0 / math.sqrt(hd)
    f32, bf16 = jnp.float32, jnp.bfloat16

    def at(index, length):
        return pl.ds(index * length if isinstance(index, int) else pl.multiple_of(index * length, length), length)

    plane = s // 2
    p = lax.rem(s, 2) * n + h
    own = p // 2
    has_up, has_down, has_two = s + 2 < seqs, s >= 2, s >= 4

    def dev(index):
        return {"seq": s - lax.rem(s, 2) + index // n, "head": lax.rem(index, n)}

    def flip(value, by):
        bit = 1
        while bit <= by:
            if (by // bit) % 2:
                value = value + bit - 2 * bit * lax.rem(value // bit, 2)
            bit *= 2
        return value

    barrier = pltpu.get_barrier_semaphore()
    for by in range(1, size):
        pl.semaphore_signal(barrier, inc=1, device_id=dev(flip(p, by)), device_id_type=MESH)

    @pl.when(has_up)
    def _():
        pl.semaphore_signal(barrier, inc=1, device_id={"seq": s + 2}, device_id_type=MESH)

    @pl.when(has_down)
    def _():
        pl.semaphore_signal(barrier, inc=1, device_id={"seq": s - 2}, device_id_type=MESH)

    pl.semaphore_wait(barrier, size - 1 + jnp.minimum(s // 2, 1) + jnp.minimum((seqs - 1 - s) // 2, 1))

    kinds = 3 + 2 * pairs

    def entry(kind, to, me):
        if kind < 2:
            dst = kvb.at[BACK + me // 2, kind, at(lax.rem(me, 2), rows), :]
            return (k_ref, v_ref)[kind].at[:, at(to, hd)], dst
        if kind == 2:
            return stl.at[to], stb.at[:, at(me, rows)]
        pair, which = (kind - 3) // 2, (kind - 3) % 2
        src = (q_ref, e_ref)[which].at[:, at(to * pairs + pair, pcols)]
        return src, (qb, eb)[which].at[at(me, rows), pl.ds(pair * pcols, pcols)]

    def entry_copy(kind, to):
        src, dst = entry(kind, to, p)
        return pltpu.make_async_remote_copy(
            src_ref=src, dst_ref=dst, send_sem=in_s.at[kind, to], recv_sem=in_r.at[kind, p],
            device_id=dev(to), device_id_type=MESH)

    def entry_got(kind, by):
        _, dst = entry(kind, p, flip(p, by))
        pltpu.make_async_remote_copy(
            src_ref=dst, dst_ref=dst, send_sem=in_s.at[kind, flip(p, by)], recv_sem=in_r.at[kind, flip(p, by)],
            device_id=dev(flip(p, by)), device_id_type=MESH).wait_recv()

    def entry_own(kind):
        src, dst = entry(kind, p, p)
        return pltpu.make_async_copy(src, dst, loc_sem.at[kind])

    order = tuple(sorted(range(1, size), key=lambda by: (by // 2 > 0, by // 2 == 3, by % 2, by)))

    for kind in (0, 1):
        loads[kind].wait()
        entry_own(kind).start()
    for by in order:
        for kind in (0, 1):
            entry_copy(kind, flip(p, by)).start()
    loads[2].wait()
    loads[3].wait()

    lane = lax.broadcasted_iota(jnp.int32, (rows, hd), 1)
    delta = jnp.zeros((rows, hd), f32)
    for head in range(width * size):
        here = pl.ds(head * hd, hd)
        one = jnp.sum(e_ref[:, here].astype(f32) * o_ref[:, here].astype(f32), axis=1, keepdims=True)
        delta = jnp.where(lane == head, one, delta)
    delta = delta.T
    loads[5].wait()
    loads[6].wait()
    for to in range(size):
        stl[to, :width, :] = lse_ref[to * width : (to + 1) * width, :] * LOG2E
        stl[to, width:, :] = delta[to * width : (to + 1) * width, :]
    entry_own(2).start()
    for by in order:
        entry_copy(2, flip(p, by)).start()
    loads[4].wait()
    for kind in range(3, kinds):
        entry_own(kind).start()
        entry_copy(kind, flip(p, 1)).start()
    def peer(base, core):
        chip = flip(p, base)
        return chip - lax.rem(chip, 2) + core

    for bases, core, pair in (
        ((2, 4), 1, 0),
        ((2, 4), 0, 0),
        ((2, 4), 1, 1),
        ((6,), 1, 0),
        ((2, 4), 0, 1),
        ((6,), 1, 1),
        ((6,), 0, 0),
        ((6,), 0, 1),
    ):
        for base in bases:
            for which in range(2):
                entry_copy(3 + 2 * pair + which, peer(base, core)).start()

    first = plane * size - BACK * 2
    for a in range(2 * window):
        row = seg_ref[pl.ds(jnp.maximum(first + a, 0), 1), :].astype(f32)
        segk[a * rows : (a + 1) * rows, :] = jnp.broadcast_to(row, (rows, hd)).T
        if a >= 2 * BACK:
            segq[:, (a - 2 * BACK) * rows : (a - 2 * BACK + 1) * rows] = row
    dqt[...] = jnp.zeros_like(dqt)
    acck[...] = jnp.zeros_like(acck)
    accv[...] = jnp.zeros_like(accv)

    def hand(w):
        return pltpu.make_async_remote_copy(
            src_ref=kvb.at[w + tiles], dst_ref=kvb.at[w], send_sem=fw_s.at[w], recv_sem=fw_r.at[w],
            device_id={"seq": s + 2}, device_id_type=MESH)

    def back(w):
        return pltpu.make_async_remote_copy(
            src_ref=ps.at[w], dst_ref=pr.at[w], send_sem=pt_s.at[w], recv_sem=pt_r.at[w],
            device_id={"seq": s - 2}, device_id_type=MESH)

    row_at = lax.broadcasted_iota(jnp.int32, (tile, tile), 0)
    col_at = lax.broadcasted_iota(jnp.int32, (tile, tile), 1)

    def work(i, w, pair):
        q_rows = at(i, tile)
        key, val = kvb[w, 0], kvb[w, 1]
        key_t = key.T
        k_seg = segk[at(w, tile), :]
        allowed = jnp.concatenate([k_seg] * (tile // hd), axis=1) == segq[:, q_rows]
        if not isinstance(w, int) or w >= BACK:
            allowed &= row_at + (w - BACK - i) * tile <= col_at
        mine = range(pair * width // pairs, (pair + 1) * width // pairs)
        queries = [qb[q_rows, m * hd : (m + 1) * hd] for m in mine]
        grads = [eb[q_rows, m * hd : (m + 1) * hd] for m in mine]
        scores = [dot_nt(key, query) for query in queries]
        dprobs = [dot_nt(val, grad) for grad in grads]
        low, dscores = [], []
        for m, score, dprob in zip(mine, scores, dprobs):
            lse = stb[m : m + 1, q_rows]
            delta = stb[width + m : width + m + 1, q_rows]
            probs = jnp.exp2(jnp.where(allowed, score * (scale * LOG2E) - lse, -jnp.inf))
            low.append(probs.astype(bf16))
            dscores.append((probs * (dprob - delta)).astype(bf16))
        accv[w] += dot(jnp.concatenate(low, axis=1), jnp.concatenate(grads, axis=0))
        acck[w] += dot(jnp.concatenate(dscores, axis=1), jnp.concatenate(queries, axis=0))
        for m, dscore in zip(mine, dscores):
            dqt[i, m] += dot(key_t, dscore)

    def leave(which, to, me):
        if which < pairs:
            src = dqs.at[at(to, rows), pl.ds(which * pcols, pcols)]
            return src, dq_out.at[:, at(me * pairs + which, pcols)]
        src, dst = ((dks, dk_out), (dvs, dv_out))[which - pairs]
        return src.at[at(to, rows), :], dst.at[:, at(me, hd)]

    leaves = pairs + 2

    def leave_copy(which, to):
        src, dst = leave(which, to, p)
        return pltpu.make_async_remote_copy(
            src_ref=src, dst_ref=dst, send_sem=out_s.at[which, to], recv_sem=out_r.at[which, p],
            device_id=dev(to), device_id_type=MESH)

    def leave_got(which, by):
        _, dst = leave(which, p, flip(p, by))
        pltpu.make_async_remote_copy(
            src_ref=dst, dst_ref=dst, send_sem=out_s.at[which, flip(p, by)], recv_sem=out_r.at[which, flip(p, by)],
            device_id=dev(flip(p, by)), device_id_type=MESH).wait_recv()

    def leave_own(which):
        src, dst = leave(which, p, p)
        return pltpu.make_async_copy(src, dst, loc_sem.at[kinds + which])

    def leave_start(which, i):
        for b in range(2):
            to = 2 * i + b

            @pl.when(to != p)
            def _():
                leave_copy(which, to).start()

            @pl.when(to == p)
            def _():
                leave_own(which).start()

    def fill(i, pair):
        for m in range(pair * width // pairs, (pair + 1) * width // pairs):
            dqs[at(i, tile), m * hd : (m + 1) * hd] = (dqt[i, m] * scale).T.astype(bf16)

    def by_twos(i, start, stop, pair):
        count = stop - start

        @pl.loop(0, count // 2)
        def _(t):
            work(i, start + 2 * t, pair)
            work(i, start + 2 * t + 1, pair)

        @pl.when(lax.rem(count, 2) == 1)
        def _():
            work(i, stop - 1, pair)

    def all_pairs(i, w):
        for pair in range(pairs):
            work(i, w, pair)

    def query_got(j, pair):
        for by in range(2 * j, 2 * j + 2):
            for kind in ((2,) if pair == 0 else ()) + (3 + 2 * pair, 4 + 2 * pair):
                entry_got(kind, by)

    def put(w):
        ps[w, 0] = acck[w].astype(bf16)
        ps[w, 1] = accv[w].astype(bf16)
        back(w).start()

    def join(w):
        back(w - tiles).wait_recv()
        acck[w] += pr[w - tiles, 0].astype(f32)
        accv[w] += pr[w - tiles, 1].astype(f32)

    for kind in range(kinds):
        entry_own(kind).wait()
    for j in range(tiles):
        for by in range(max(2 * j, 1), 2 * j + 2):
            entry_got(0, by)
            entry_got(1, by)
        t = flip(own, j)

        @pl.when(has_up)
        def _():
            hand(t + BACK - tiles).start()

        if j == 0:
            for kind in range(2, kinds):
                entry_got(kind, 1)

        @pl.when(t <= own)
        def _():
            all_pairs(own, t + BACK)

    last = tiles - 1
    far = flip(own, last)

    def before(j):
        w = BACK - tiles + flip(own, j)

        @pl.when(has_down)
        def _():
            hand(w).wait_recv()

            @pl.when(has_up & (w >= tiles))
            def _():
                hand(w - tiles).start()

            @pl.when(own <= w)
            def _():
                all_pairs(own, w)

    sides = [flip(own, j) for j in range(1, last)]

    def near(w, pair):
        for i in sides:
            if w >= tiles - 1:
                work(i, w, pair)
            else:
                @pl.when(i <= w)
                def _():
                    work(i, w, pair)

    for j in range(last - 1):
        before(j)
    for pair in range(pairs):
        for j in range(1, last):
            query_got(j, pair)
            i = flip(own, j)
            if pair == 0:
                by_twos(i, BACK, i + BACK + 1, pair)

        if pair == 0:
            for j in range(last - 1, tiles):
                before(j)

        @pl.when(has_down)
        def _():
            for w in range(BACK - tiles, BACK):
                near(w, pair)

    @pl.when(has_two)
    def _():
        for w in range(BACK - tiles - 1, -1, -1):
            hand(w).wait_recv()

            @pl.loop(0, w + 1)
            def _(i):
                @pl.when(i != far)
                def _():
                    all_pairs(i, w)

    for pair in range(pairs):
        fill(own, pair)
    for i in sides:
        fill(i, 0)
        leave_start(0, i)

    for w in range(last):
        @pl.when((has_two if w < BACK - tiles else has_down) & (far > w))
        def _():
            put(w)

    bottom = jnp.maximum(far, jnp.maximum(BACK - tiles * plane, 0))
    for pair in range(pairs - 1):
        query_got(last, pair)
        by_twos(far, jnp.minimum(bottom, BACK), BACK, pair)
    query_got(last, pairs - 1)

    def rest(*some):
        for w in some:
            work(far, w, pairs - 1)
        for w in some:
            @pl.when(w < tiles)
            def _():
                put(w)

    @pl.when(has_two)
    def _():
        for w in range(0, BACK - tiles, 2):
            @pl.when(far <= w)
            def _():
                rest(w, w + 1)

            @pl.when(far == w + 1)
            def _():
                rest(w + 1)

    turns = tuple(range(tiles - 1, -1, -1))
    ws = [BACK - tiles + flip(own, j) for j in turns]

    @pl.when(has_down)
    def _():
        rest(*ws[:2])

        @pl.when(far <= ws[3])
        def _():
            rest(*ws[2:])

        @pl.when(far > ws[3])
        def _():
            rest(ws[2])

    for pair in range(pairs):
        leave_start(pair, own)
    for i in sides:
        for pair in range(1, pairs):
            by_twos(i, BACK, i + BACK + 1, pair)
            fill(i, pair)
            leave_start(pair, i)

    @pl.loop(BACK, far + BACK + 1)
    def _(w):
        all_pairs(far, w)

    for pair in range(pairs):
        fill(far, pair)
        leave_start(pair, far)

    @pl.when(has_down)
    def _():
        for w in ws:
            @pl.when(w >= tiles)
            def _():
                @pl.when(has_up)
                def _():
                    join(w)

                put(w)

    for j in turns:
        t = flip(own, j)
        w = t + BACK

        @pl.when(has_up)
        def _():
            join(w)

        dks[at(t, tile), :] = (acck[w] * scale).astype(bf16)
        dvs[at(t, tile), :] = accv[w].astype(bf16)
        leave_start(pairs, t)
        leave_start(pairs + 1, t)

    for which in range(leaves):
        leave_own(which).wait()
        for by in range(1, size):
            leave_got(which, by)
            leave_copy(which, flip(p, by)).wait_send()
    for kind in range(kinds):
        for by in range(1, size):
            entry_copy(kind, flip(p, by)).wait_send()
    for w in range(BACK):
        low = w < BACK - tiles

        @pl.when(has_up & has_down if low else has_up)
        def _():
            hand(w).wait_send()

        @pl.when(has_two if low else has_down)
        def _():
            back(w).wait_send()


def move(*refs):
    ins, outs, sems = refs[:3], refs[3:6], refs[6]
    copies = [pltpu.make_async_copy(a, b, sems.at[at]) for at, (a, b) in enumerate(zip(ins, outs))]
    for copy in copies:
        copy.start()
    for copy in copies:
        copy.wait()


def shards(query, key, value, out, output_gradient, log_sum_exp, segment_ids):
    n, seqs = lax.axis_size("head"), lax.axis_size("seq")
    hd = HEAD_SIZE
    rows = query.shape[0]
    size = 2 * n
    cols = query.shape[1] // size
    width = cols // hd
    pairs = width // 2
    tile, tiles = 2 * rows, size // 2
    window = tiles + BACK
    bf16, f32 = jnp.bfloat16, jnp.float32
    kinds, leaves = 3 + 2 * pairs, pairs + 2
    vmem = pl.BlockSpec(memory_space=pltpu.VMEM)
    dma = pltpu.SemaphoreType.DMA
    anywhere = pl.BlockSpec(memory_space=pl.ANY)
    parts = pl.pallas_call(
        functools.partial(kernel, n, seqs, width),
        out_shape=[pltpu.VMEM(like.shape, bf16) for like in (query, key, value)],
        in_specs=[anywhere] * 7,
        out_specs=[vmem] * 3,
        scratch_shapes=[
            pltpu.VMEM(key.shape, bf16),
            pltpu.VMEM(value.shape, bf16),
            pltpu.VMEM(query.shape, bf16),
            pltpu.VMEM(query.shape, bf16),
            pltpu.VMEM(query.shape, bf16),
            pltpu.VMEM(log_sum_exp.shape[::-1], f32),
            pltpu.VMEM((segment_ids.size // hd, hd), jnp.int32),
            dma((7,)),
            pltpu.VMEM((size * rows, cols), bf16),
            pltpu.VMEM((size * rows, cols), bf16),
            pltpu.VMEM((size, 2 * width, rows), f32),
            pltpu.VMEM((2 * width, size * rows), f32),
            pltpu.VMEM((window, 2, tile, hd), bf16),
            pltpu.VMEM((window * tile, hd), f32),
            pltpu.VMEM((1, size * rows), f32),
            pltpu.VMEM((tiles, width, hd, tile), f32),
            pltpu.VMEM((window, tile, hd), f32),
            pltpu.VMEM((window, tile, hd), f32),
            pltpu.VMEM((BACK, 2, tile, hd), bf16),
            pltpu.VMEM((BACK, 2, tile, hd), bf16),
            pltpu.VMEM((size * rows, cols), bf16),
            pltpu.VMEM((size * rows, hd), bf16),
            pltpu.VMEM((size * rows, hd), bf16),
            dma((kinds + leaves,)),
            dma((kinds, size)),
            dma((kinds, size)),
            dma((BACK,)),
            dma((BACK,)),
            dma((BACK,)),
            dma((BACK,)),
            dma((leaves, size)),
            dma((leaves, size)),
        ],
        compiler_params=pltpu.CompilerParams(collective_id=0, has_side_effects=True),
    )(query, output_gradient, out, key, value, log_sum_exp.T, segment_ids.reshape(-1, hd))
    return pl.pallas_call(
        move,
        out_shape=[jax.ShapeDtypeStruct(part.shape, bf16) for part in parts],
        in_specs=[vmem] * 3,
        out_specs=[anywhere] * 3,
        scratch_shapes=[dma((3,))],
        compiler_params=pltpu.CompilerParams(vmem_limit_bytes=1 << 20),
    )(*parts)


def solution(mesh):
    placed = (P(("seq", "head"), None),) * 6 + (P(),)
    return jax.shard_map(
        lambda *a: tuple(shards(*a)),
        mesh=mesh,
        in_specs=placed,
        out_specs=(P(("seq", "head"), None),) * 3,
        check_vma=False,
    )
```

```python
import functools
import math

import jax
import jax.numpy as jnp
from jax import lax
from jax.experimental import pallas as pl
from jax.experimental.pallas import tpu as pltpu
from jax.sharding import PartitionSpec as P

HEAD_SIZE = 128
BACK = 6
LOG2E = math.log2(math.e)
MESH = pl.DeviceIdType.MESH
NT = (((1,), (1,)), ((), ()))


def dot(a, b):
    return jnp.dot(a, b, preferred_element_type=jnp.float32)


def dot_nt(a, b):
    return lax.dot_general(a, b, NT, preferred_element_type=jnp.float32)


def kernel(
    n, seqs, width,
    q_in, e_in, o_in, k_in, v_in, lse_in, seg_in,
    dq_out, dk_out, dv_out,
    k_ref, v_ref, e_ref, o_ref, q_ref, lse_ref, seg_ref, load_sem, qb, eb, stl, stb, kvb, segk, segq, dqt, acck, accv, ps, pr, dqs, dks, dvs,
    loc_sem, in_s, in_r, fw_s, fw_r, pt_s, pt_r, out_s, out_r,
):
    s = lax.axis_index("seq")
    h = lax.axis_index("head")
    rows = q_ref.shape[0]
    hd = HEAD_SIZE
    loads = [
        pltpu.make_async_copy(src, dst, load_sem.at[at])
        for at, (src, dst) in enumerate((
            (k_in, k_ref), (v_in, v_ref), (e_in, e_ref), (o_in, o_ref), (q_in, q_ref), (lse_in, lse_ref), (seg_in, seg_ref),
        ))
    ]
    for load in loads:
        load.start()
    tile = 2 * rows
    size = 2 * n
    tiles = size // 2
    window = tiles + BACK
    cols = width * hd
    pairs = width // 2
    pcols = cols // pairs
    scale = 1.0 / math.sqrt(hd)
    f32, bf16 = jnp.float32, jnp.bfloat16

    def at(index, length):
        return pl.ds(index * length if isinstance(index, int) else pl.multiple_of(index * length, length), length)

    plane = s // 2
    p = lax.rem(s, 2) * n + h
    own = p // 2
    has_up, has_down, has_two = s + 2 < seqs, s >= 2, s >= 4

    def dev(index):
        return {"seq": s - lax.rem(s, 2) + index // n, "head": lax.rem(index, n)}

    def flip(value, by):
        bit = 1
        while bit <= by:
            if (by // bit) % 2:
                value = value + bit - 2 * bit * lax.rem(value // bit, 2)
            bit *= 2
        return value

    barrier = pltpu.get_barrier_semaphore()
    for by in range(1, size):
        pl.semaphore_signal(barrier, inc=1, device_id=dev(flip(p, by)), device_id_type=MESH)

    @pl.when(has_up)
    def _():
        pl.semaphore_signal(barrier, inc=1, device_id={"seq": s + 2}, device_id_type=MESH)

    @pl.when(has_down)
    def _():
        pl.semaphore_signal(barrier, inc=1, device_id={"seq": s - 2}, device_id_type=MESH)

    pl.semaphore_wait(barrier, size - 1 + jnp.minimum(s // 2, 1) + jnp.minimum((seqs - 1 - s) // 2, 1))

    kinds = 3 + 2 * pairs

    def entry(kind, to, me):
        if kind < 2:
            dst = kvb.at[BACK + me // 2, kind, at(lax.rem(me, 2), rows), :]
            return (k_ref, v_ref)[kind].at[:, at(to, hd)], dst
        if kind == 2:
            return stl.at[to], stb.at[:, at(me, rows)]
        pair, which = (kind - 3) // 2, (kind - 3) % 2
        src = (q_ref, e_ref)[which].at[:, at(to * pairs + pair, pcols)]
        return src, (qb, eb)[which].at[at(me, rows), pl.ds(pair * pcols, pcols)]

    def entry_copy(kind, to):
        src, dst = entry(kind, to, p)
        return pltpu.make_async_remote_copy(
            src_ref=src, dst_ref=dst, send_sem=in_s.at[kind, to], recv_sem=in_r.at[kind, p],
            device_id=dev(to), device_id_type=MESH)

    def entry_got(kind, by):
        _, dst = entry(kind, p, flip(p, by))
        pltpu.make_async_remote_copy(
            src_ref=dst, dst_ref=dst, send_sem=in_s.at[kind, flip(p, by)], recv_sem=in_r.at[kind, flip(p, by)],
            device_id=dev(flip(p, by)), device_id_type=MESH).wait_recv()

    def entry_own(kind):
        src, dst = entry(kind, p, p)
        return pltpu.make_async_copy(src, dst, loc_sem.at[kind])

    order = tuple(sorted(range(1, size), key=lambda by: (by // 2 > 0, by // 2 == 3, by % 2, by)))

    for kind in (0, 1):
        loads[kind].wait()
        entry_own(kind).start()
    for by in order:
        for kind in (0, 1):
            entry_copy(kind, flip(p, by)).start()
    loads[2].wait()
    loads[3].wait()

    lane = lax.broadcasted_iota(jnp.int32, (rows, hd), 1)
    delta = jnp.zeros((rows, hd), f32)
    for head in range(width * size):
        here = pl.ds(head * hd, hd)
        one = jnp.sum(e_ref[:, here].astype(f32) * o_ref[:, here].astype(f32), axis=1, keepdims=True)
        delta = jnp.where(lane == head, one, delta)
    delta = delta.T
    loads[5].wait()
    loads[6].wait()
    for to in range(size):
        stl[to, :width, :] = lse_ref[to * width : (to + 1) * width, :] * LOG2E
        stl[to, width:, :] = delta[to * width : (to + 1) * width, :]
    entry_own(2).start()
    for by in order:
        entry_copy(2, flip(p, by)).start()
    loads[4].wait()
    for kind in range(3, kinds):
        entry_own(kind).start()
        entry_copy(kind, flip(p, 1)).start()
    def peer(base, core):
        chip = flip(p, base)
        return chip - lax.rem(chip, 2) + core

    for bases, core, pair in (
        ((2, 4), 1, 0),
        ((2, 4), 0, 0),
        ((2, 4), 1, 1),
        ((2, 4), 0, 1),
        ((6,), 1, 0),
        ((6,), 1, 1),
        ((6,), 0, 0),
        ((6,), 0, 1),
    ):
        for base in bases:
            for which in range(2):
                entry_copy(3 + 2 * pair + which, peer(base, core)).start()

    first = plane * size - BACK * 2
    for a in range(2 * window):
        row = seg_ref[pl.ds(jnp.maximum(first + a, 0), 1), :].astype(f32)
        segk[a * rows : (a + 1) * rows, :] = jnp.broadcast_to(row, (rows, hd)).T
        if a >= 2 * BACK:
            segq[:, (a - 2 * BACK) * rows : (a - 2 * BACK + 1) * rows] = row
    dqt[...] = jnp.zeros_like(dqt)
    acck[...] = jnp.zeros_like(acck)
    accv[...] = jnp.zeros_like(accv)

    def hand(w):
        return pltpu.make_async_remote_copy(
            src_ref=kvb.at[w + tiles], dst_ref=kvb.at[w], send_sem=fw_s.at[w], recv_sem=fw_r.at[w],
            device_id={"seq": s + 2}, device_id_type=MESH)

    def back(w):
        return pltpu.make_async_remote_copy(
            src_ref=ps.at[w], dst_ref=pr.at[w], send_sem=pt_s.at[w], recv_sem=pt_r.at[w],
            device_id={"seq": s - 2}, device_id_type=MESH)

    row_at = lax.broadcasted_iota(jnp.int32, (tile, tile), 0)
    col_at = lax.broadcasted_iota(jnp.int32, (tile, tile), 1)

    def work(i, w, pair):
        q_rows = at(i, tile)
        key, val = kvb[w, 0], kvb[w, 1]
        key_t = key.T
        k_seg = segk[at(w, tile), :]
        allowed = jnp.concatenate([k_seg] * (tile // hd), axis=1) == segq[:, q_rows]
        if not isinstance(w, int) or w >= BACK:
            allowed &= row_at + (w - BACK - i) * tile <= col_at
        mine = range(pair * width // pairs, (pair + 1) * width // pairs)
        queries = [qb[q_rows, m * hd : (m + 1) * hd] for m in mine]
        grads = [eb[q_rows, m * hd : (m + 1) * hd] for m in mine]
        scores = [dot_nt(key, query) for query in queries]
        dprobs = [dot_nt(val, grad) for grad in grads]
        low, dscores = [], []
        for m, score, dprob in zip(mine, scores, dprobs):
            lse = stb[m : m + 1, q_rows]
            delta = stb[width + m : width + m + 1, q_rows]
            probs = jnp.exp2(jnp.where(allowed, score * (scale * LOG2E) - lse, -jnp.inf))
            low.append(probs.astype(bf16))
            dscores.append((probs * (dprob - delta)).astype(bf16))
        accv[w] += dot(jnp.concatenate(low, axis=1), jnp.concatenate(grads, axis=0))
        acck[w] += dot(jnp.concatenate(dscores, axis=1), jnp.concatenate(queries, axis=0))
        for m, dscore in zip(mine, dscores):
            dqt[i, m] += dot(key_t, dscore)

    def leave(which, to, me):
        if which < pairs:
            src = dqs.at[at(to, rows), pl.ds(which * pcols, pcols)]
            return src, dq_out.at[:, at(me * pairs + which, pcols)]
        src, dst = ((dks, dk_out), (dvs, dv_out))[which - pairs]
        return src.at[at(to, rows), :], dst.at[:, at(me, hd)]

    leaves = pairs + 2

    def leave_copy(which, to):
        src, dst = leave(which, to, p)
        return pltpu.make_async_remote_copy(
            src_ref=src, dst_ref=dst, send_sem=out_s.at[which, to], recv_sem=out_r.at[which, p],
            device_id=dev(to), device_id_type=MESH)

    def leave_got(which, by):
        _, dst = leave(which, p, flip(p, by))
        pltpu.make_async_remote_copy(
            src_ref=dst, dst_ref=dst, send_sem=out_s.at[which, flip(p, by)], recv_sem=out_r.at[which, flip(p, by)],
            device_id=dev(flip(p, by)), device_id_type=MESH).wait_recv()

    def leave_own(which):
        src, dst = leave(which, p, p)
        return pltpu.make_async_copy(src, dst, loc_sem.at[kinds + which])

    def leave_start(which, i):
        for b in range(2):
            to = 2 * i + b

            @pl.when(to != p)
            def _():
                leave_copy(which, to).start()

            @pl.when(to == p)
            def _():
                leave_own(which).start()

    def fill(i, pair):
        for m in range(pair * width // pairs, (pair + 1) * width // pairs):
            dqs[at(i, tile), m * hd : (m + 1) * hd] = (dqt[i, m] * scale).T.astype(bf16)

    def by_twos(i, start, stop, pair):
        count = stop - start

        @pl.loop(0, count // 2)
        def _(t):
            work(i, start + 2 * t, pair)
            work(i, start + 2 * t + 1, pair)

        @pl.when(lax.rem(count, 2) == 1)
        def _():
            work(i, stop - 1, pair)

    def all_pairs(i, w):
        for pair in range(pairs):
            work(i, w, pair)

    def query_got(j, pair):
        for by in range(2 * j, 2 * j + 2):
            for kind in ((2,) if pair == 0 else ()) + (3 + 2 * pair, 4 + 2 * pair):
                entry_got(kind, by)

    def put(w):
        ps[w, 0] = acck[w].astype(bf16)
        ps[w, 1] = accv[w].astype(bf16)
        back(w).start()

    def join(w):
        back(w - tiles).wait_recv()
        acck[w] += pr[w - tiles, 0].astype(f32)
        accv[w] += pr[w - tiles, 1].astype(f32)

    for kind in range(kinds):
        entry_own(kind).wait()
    for j in range(tiles):
        for by in range(max(2 * j, 1), 2 * j + 2):
            entry_got(0, by)
            entry_got(1, by)
        t = flip(own, j)

        @pl.when(has_up)
        def _():
            hand(t + BACK - tiles).start()

        if j == 0:
            for kind in range(2, kinds):
                entry_got(kind, 1)

        @pl.when(t <= own)
        def _():
            all_pairs(own, t + BACK)

    last = tiles - 1
    far = flip(own, last)

    def before(j):
        w = BACK - tiles + flip(own, j)

        @pl.when(has_down)
        def _():
            hand(w).wait_recv()

            @pl.when(has_up & (w >= tiles))
            def _():
                hand(w - tiles).start()

            @pl.when(own <= w)
            def _():
                all_pairs(own, w)

    sides = [flip(own, j) for j in range(1, last)]

    def near(w, pair):
        for i in sides:
            if w >= tiles - 1:
                work(i, w, pair)
            else:
                @pl.when(i <= w)
                def _():
                    work(i, w, pair)

    for j in range(last - 1):
        before(j)
    for pair in range(pairs):
        for j in range(1, last):
            query_got(j, pair)
            i = flip(own, j)
            if pair == 0:
                by_twos(i, BACK, i + BACK + 1, pair)

        if pair == 0:
            for j in range(last - 1, tiles):
                before(j)

        @pl.when(has_down)
        def _():
            for w in range(BACK - tiles, BACK):
                near(w, pair)

    @pl.when(has_two)
    def _():
        for w in range(BACK - tiles - 1, -1, -1):
            hand(w).wait_recv()

            @pl.loop(0, w + 1)
            def _(i):
                @pl.when(i != far)
                def _():
                    all_pairs(i, w)

    for pair in range(pairs):
        fill(own, pair)
    for i in sides:
        fill(i, 0)
        leave_start(0, i)

    def side_rest():
        for i in sides:
            for pair in range(1, pairs):
                by_twos(i, BACK, i + BACK + 1, pair)
                fill(i, pair)
                leave_start(pair, i)

    late_core = lax.rem(p, 2) == 0

    @pl.when(late_core)
    def _():
        side_rest()

    for w in range(last):
        @pl.when((has_two if w < BACK - tiles else has_down) & (far > w))
        def _():
            put(w)

    bottom = jnp.maximum(far, jnp.maximum(BACK - tiles * plane, 0))
    for pair in range(pairs - 1):
        query_got(last, pair)
        by_twos(far, jnp.minimum(bottom, BACK), BACK, pair)
    query_got(last, pairs - 1)

    def rest(*some):
        for w in some:
            work(far, w, pairs - 1)
        for w in some:
            @pl.when(w < tiles)
            def _():
                put(w)

    @pl.when(has_two)
    def _():
        for w in range(0, BACK - tiles, 2):
            @pl.when(far <= w)
            def _():
                rest(w, w + 1)

            @pl.when(far == w + 1)
            def _():
                rest(w + 1)

    turns = tuple(range(tiles - 1, -1, -1))
    ws = [BACK - tiles + flip(own, j) for j in turns]

    @pl.when(has_down)
    def _():
        rest(*ws[:2])

        @pl.when(far <= ws[3])
        def _():
            rest(*ws[2:])

        @pl.when(far > ws[3])
        def _():
            rest(ws[2])

    for pair in range(pairs):
        leave_start(pair, own)
    @pl.when(jnp.logical_not(late_core))
    def _():
        side_rest()

    @pl.loop(BACK, far + BACK + 1)
    def _(w):
        all_pairs(far, w)

    for pair in range(pairs):
        fill(far, pair)
        leave_start(pair, far)

    @pl.when(has_down)
    def _():
        for w in ws:
            @pl.when(w >= tiles)
            def _():
                @pl.when(has_up)
                def _():
                    join(w)

                put(w)

    for j in turns:
        t = flip(own, j)
        w = t + BACK

        @pl.when(has_up)
        def _():
            join(w)

        dks[at(t, tile), :] = (acck[w] * scale).astype(bf16)
        dvs[at(t, tile), :] = accv[w].astype(bf16)
        leave_start(pairs, t)
        leave_start(pairs + 1, t)

    for which in range(leaves):
        leave_own(which).wait()
        for by in range(1, size):
            leave_got(which, by)
            leave_copy(which, flip(p, by)).wait_send()
    for kind in range(kinds):
        for by in range(1, size):
            entry_copy(kind, flip(p, by)).wait_send()
    for w in range(BACK):
        low = w < BACK - tiles

        @pl.when(has_up & has_down if low else has_up)
        def _():
            hand(w).wait_send()

        @pl.when(has_two if low else has_down)
        def _():
            back(w).wait_send()


def move(*refs):
    ins, outs, sems = refs[:3], refs[3:6], refs[6]
    copies = [pltpu.make_async_copy(a, b, sems.at[at]) for at, (a, b) in enumerate(zip(ins, outs))]
    for copy in copies:
        copy.start()
    for copy in copies:
        copy.wait()


def shards(query, key, value, out, output_gradient, log_sum_exp, segment_ids):
    n, seqs = lax.axis_size("head"), lax.axis_size("seq")
    hd = HEAD_SIZE
    rows = query.shape[0]
    size = 2 * n
    cols = query.shape[1] // size
    width = cols // hd
    pairs = width // 2
    tile, tiles = 2 * rows, size // 2
    window = tiles + BACK
    bf16, f32 = jnp.bfloat16, jnp.float32
    kinds, leaves = 3 + 2 * pairs, pairs + 2
    vmem = pl.BlockSpec(memory_space=pltpu.VMEM)
    dma = pltpu.SemaphoreType.DMA
    anywhere = pl.BlockSpec(memory_space=pl.ANY)
    parts = pl.pallas_call(
        functools.partial(kernel, n, seqs, width),
        out_shape=[pltpu.VMEM(like.shape, bf16) for like in (query, key, value)],
        in_specs=[anywhere] * 7,
        out_specs=[vmem] * 3,
        scratch_shapes=[
            pltpu.VMEM(key.shape, bf16),
            pltpu.VMEM(value.shape, bf16),
            pltpu.VMEM(query.shape, bf16),
            pltpu.VMEM(query.shape, bf16),
            pltpu.VMEM(query.shape, bf16),
            pltpu.VMEM(log_sum_exp.shape[::-1], f32),
            pltpu.VMEM((segment_ids.size // hd, hd), jnp.int32),
            dma((7,)),
            pltpu.VMEM((size * rows, cols), bf16),
            pltpu.VMEM((size * rows, cols), bf16),
            pltpu.VMEM((size, 2 * width, rows), f32),
            pltpu.VMEM((2 * width, size * rows), f32),
            pltpu.VMEM((window, 2, tile, hd), bf16),
            pltpu.VMEM((window * tile, hd), f32),
            pltpu.VMEM((1, size * rows), f32),
            pltpu.VMEM((tiles, width, hd, tile), f32),
            pltpu.VMEM((window, tile, hd), f32),
            pltpu.VMEM((window, tile, hd), f32),
            pltpu.VMEM((BACK, 2, tile, hd), bf16),
            pltpu.VMEM((BACK, 2, tile, hd), bf16),
            pltpu.VMEM((size * rows, cols), bf16),
            pltpu.VMEM((size * rows, hd), bf16),
            pltpu.VMEM((size * rows, hd), bf16),
            dma((kinds + leaves,)),
            dma((kinds, size)),
            dma((kinds, size)),
            dma((BACK,)),
            dma((BACK,)),
            dma((BACK,)),
            dma((BACK,)),
            dma((leaves, size)),
            dma((leaves, size)),
        ],
        compiler_params=pltpu.CompilerParams(collective_id=0, has_side_effects=True),
    )(query, output_gradient, out, key, value, log_sum_exp.T, segment_ids.reshape(-1, hd))
    return pl.pallas_call(
        move,
        out_shape=[jax.ShapeDtypeStruct(part.shape, bf16) for part in parts],
        in_specs=[vmem] * 3,
        out_specs=[anywhere] * 3,
        scratch_shapes=[dma((3,))],
        compiler_params=pltpu.CompilerParams(vmem_limit_bytes=1 << 20),
    )(*parts)


def solution(mesh):
    placed = (P(("seq", "head"), None),) * 6 + (P(),)
    return jax.shard_map(
        lambda *a: tuple(shards(*a)),
        mesh=mesh,
        in_specs=placed,
        out_specs=(P(("seq", "head"), None),) * 3,
        check_vma=False,
    )
```
